128 devices in a mesh: blk: 64 (over x, y, z_lo, core), grp: 2 (over z_hi).
Axes of the slice: x: 4, y: 4, z: 4 (z_hi: 2, z_lo: 2; z = z_hi * 2 + z_lo), core: 2. Of those that a mesh axis runs over, the one named last changes fastest.
Arguments:
- sky_maps: float32 [4, 512, 4096], P(None, ('blk', 'grp')), may hold values from -6 to 6
- legendre: bfloat16 [512, 512, 2048], P(('blk', 'grp')), may hold values from -0.25 to 0.25
- owner_table: int32 [512], replicated, may hold values from 0 to 511, each once
Outputs:
- harmonics: float32 [512, 4, 2, 2048], P(('blk', 'grp'))
- spectra: float32 [10, 2048], P(None, ('blk', 'grp'))
The draws below stay inside these ranges and needn't reach their ends.
Inputs may be any that keep to these rules, and one draw needn't show every extreme that they name: `owner_table`: a permutation of the orders 0 to 511.
All inputs are finite; a program needn't handle non-finite values.
Results may differ from the reference program's by a relative error of at most 0.0034.
Values may be sent and summed in bfloat16 or wider, within the bound.
A program may use at most 128 MiB of HBM per device.

```python
import math
import jax
import jax.numpy as jnp
import numpy as np
from jax import lax

MAPS = 4
M = 512
L = 2048
NPHI = 4096
CYCLES = 512


def levels(own_key, shape, shards, smallest, top_value):
    def one(dim, blocks):
        heights = jax.random.uniform(jax.random.fold_in(jax.random.fold_in(own_key, 6), dim), (blocks,), jnp.float32, smallest / len(shards), top_value / len(shards))
        return jnp.repeat(jnp.exp(heights), shape[dim] // blocks).reshape((-1,) + (1,) * (len(shape) - dim - 1))

    loudness = one(*shards[0])
    for cut in shards[1:]:
        loudness = loudness * one(*cut)
    return loudness


def scatter_about(own_key, dims, scale, limit, pieces=(), kind=jnp.bfloat16):
    array = scale * jax.random.normal(own_key, dims, jnp.float32)
    if pieces:
        array = array * levels(own_key, dims, pieces, -0.22, 0.18)
    return jnp.clip(array, -limit, limit).astype(kind)


def setup_inputs(seed: int = 0) -> dict:
    seeds = jax.random.split(jax.random.key(seed), 4)
    sky_maps = scatter_about(seeds[0], (MAPS, CYCLES, NPHI), 1.0, 6.0, ((1, 128),), jnp.float32)
    legendre = scatter_about(seeds[1], (CYCLES, M, L), CYCLES ** -0.5, 0.25, ((0, 128),))
    owner_table = jax.random.permutation(seeds[2], M).astype(jnp.int32)
    return dict(sky_maps=sky_maps, legendre=legendre, owner_table=owner_table)


def reference(sky_maps, legendre, owner_table):
    coeffs = jnp.fft.rfft(sky_maps, axis=-1)[..., :M] / math.sqrt(NPHI)
    fourier = jnp.stack([jnp.real(coeffs), jnp.imag(coeffs)], axis=2)
    fourier = jnp.transpose(fourier, (1, 0, 2, 3)).reshape(CYCLES, 2 * MAPS, M).astype(jnp.bfloat16)
    ell_index = jnp.arange(L, dtype=jnp.int32)

    def per_block(orders):
        table = jnp.take(legendre, orders, axis=1).astype(jnp.float32)
        values = jnp.take(fourier, orders, axis=2).astype(jnp.float32)
        block = jnp.einsum('rcm,rml->mcl', values, table)
        keep = ell_index[None, None, :] >= orders[:, None, None]
        return jnp.where(keep, block, jnp.zeros_like(block))
    harmonics = lax.map(per_block, owner_table.reshape(M // 64, 64)).reshape(M, MAPS, 2, L)
    weight = jnp.where(owner_table == 0, jnp.float32(1.0), jnp.float32(2.0)).astype(jnp.float32)
    cross = jnp.einsum('m,miql,mjql->ijl', weight, harmonics, harmonics)
    first, second = np.triu_indices(MAPS)
    spectra = cross[first, second] / (2 * ell_index + 1).astype(jnp.float32)
    return (harmonics, spectra)
```

```python
import functools
import math

import jax
import jax.numpy as jnp
import numpy as np
from jax import lax
from jax.experimental import pallas as pl
from jax.experimental.pallas import tpu as pltpu
from jax.sharding import PartitionSpec as P

MESH = pl.DeviceIdType.MESH
F32 = jnp.float32
BF16 = jnp.bfloat16
UNITS = 16
PARTS = 6
LANES = 128


def iota(shape, dim):
    return lax.broadcasted_iota(jnp.int32, shape, dim)


def dft_tables():
    k2 = np.arange(128)[:, None]
    m = np.arange(512)[None, :]
    angle = 2.0 * math.pi * ((k2 * m) % 4096) / 4096.0
    table = np.concatenate([np.cos(angle), -np.sin(angle)], axis=1) / 64.0
    k1 = np.arange(32)[:, None]
    turn = 2.0 * math.pi * ((k1 * m) % 32) / 32.0
    twiddle = np.stack([np.cos(turn), np.sin(turn)], axis=1)
    return table.astype(np.float32), twiddle.astype(np.float32)


def kernel(
    sky_ref, leg_ref, own_ref, table_ref, twid_ref, harm_ref, spec_ref,
    legv, sendb, recvb, perm, hot, amat, fx, fz, fre, fown, frecv,
    acc, passb, passr, acc2, s2, r2, acc3, s3, r3, sp1, r1s, sp2, r2s, morder, mweight,
    leg_sem, a_send, a_recv, f_send, f_recv, b_send, b_recv, c_send, c_recv,
    d_send, d_recv, e_send, e_recv, g_send, g_recv,
):
    blk = lax.axis_index("blk")
    grp = lax.axis_index("grp")
    x = blk // 16
    y = (blk // 4) % 4
    z = grp * 2 + (blk // 2) % 2
    core = blk % 2

    def pick(axis, v0, v1, v2):
        return jnp.where(axis == 0, v0, jnp.where(axis == 1, v1, v2))

    def coords(axis):
        return pick(axis, x, y, z), pick(axis, y, z, x), pick(axis, z, x, y)

    def device(xx, yy, zz, cc):
        return (xx * 16 + yy * 4 + (zz % 2) * 2 + cc, zz // 2)

    def at(axis, v1, v2, v3, cc):
        return device(pick(axis, v1, v3, v2), pick(axis, v2, v1, v3), pick(axis, v3, v2, v1), cc)

    def part_of(u):
        part = u % PARTS
        return part, part // 2, part % 2

    def pairs(axis, par):
        a1, a2, a3 = coords(axis)
        step = (1 - 2 * (a1 % 2)) * (1 - 2 * par)
        first = (a1 + step + 4) % 4
        second = (a1 - step + 4) % 4
        return a1, a2, a3, first, second

    def remote(src, dst, ss, rs, dev):
        return pltpu.make_async_remote_copy(
            src_ref=src, dst_ref=dst, send_sem=ss, recv_sem=rs, device_id=dev, device_id_type=MESH
        )

    def loop(lo, hi, f):
        def body(i, c):
            f(i)
            return c

        lax.fori_loop(lo, hi, body, 0)

    def leg_copy(u):
        lanes = pl.ds(pl.multiple_of(u * LANES, LANES), LANES)
        return pltpu.make_async_copy(leg_ref.at[:, :, lanes], legv.at[u], leg_sem.at[u])

    loop(0, UNITS, lambda u: leg_copy(u).start())

    def hot_rows(i):
        rows = pl.ds(pl.multiple_of(i * 128, 128), 128)
        same = iota((128, 512), 0) + i * 128 == own_ref[...]
        hot[rows, :] = jnp.where(same, 1.0, 0.0).astype(BF16)

    loop(0, 4, hot_rows)

    def perm_rows(axis):
        a1, a2, a3 = coords(axis)
        step = 1 - 2 * (a1 % 2)
        i = iota((512, 512), 0)
        j = i & 3
        v3 = (a3 + (i >> 2)) & 3
        v2 = (a2 + (i >> 4)) & 3
        cc = core ^ ((i >> 6) & 1)
        v1 = (a1 + ((i >> 7) + 1) * step + 16) & 3
        xx = pick(axis, v1, v3, v2)
        yy = pick(axis, v2, v1, v3)
        zz = pick(axis, v3, v2, v1)
        slot = ((((xx * 4 + yy) * 2 + (zz & 1)) * 2 + cc) * 2 + (zz >> 1)) * 4 + j
        chosen = jnp.where(slot == iota((512, 512), 1), 1.0, 0.0).astype(BF16)
        rows = lax.dot_general(
            chosen, hot[...], (((1,), (1,)), ((), ())), preferred_element_type=F32
        )
        perm[axis] = rows.astype(BF16)

    loop(0, 3, perm_rows)

    def a_copies(u):
        part, axis, par = part_of(u)
        a1, a2, a3, first, _ = pairs(axis, par)
        return (
            remote(sendb.at[u, 1, pl.ds(2, 2)], recvb.at[u, 0], a_send.at[u, 0], a_recv.at[u, 0],
                   at(axis, a1, a2, a3, 1 - core)),
            remote(sendb.at[u, 0, pl.ds(0, 2)], recvb.at[u, 1], a_send.at[u, 1], a_recv.at[u, 1],
                   at(axis, first, a2, a3, core)),
            remote(sendb.at[u, 1, pl.ds(0, 2)], recvb.at[u, 2], a_send.at[u, 2], a_recv.at[u, 2],
                   at(axis, first, a2, a3, 1 - core)),
        )

    def phase_a(u):
        part, axis, par = part_of(u)
        leg_copy(u).wait()
        roles = (3 * par, 1, 3 - 3 * par, 2)
        for pair in range(2):
            wide = jnp.concatenate([legv[u, 2 * pair], legv[u, 2 * pair + 1]], axis=1)
            rows = jnp.dot(perm[axis], wide, preferred_element_type=F32).astype(BF16)
            for rel in range(4):
                for rc in range(2):
                    piece = rows[rel * 128 + rc * 64 : rel * 128 + rc * 64 + 64]
                    sendb[u, rc, roles[rel], 2 * pair] = piece[:, :128]
                    sendb[u, rc, roles[rel], 2 * pair + 1] = piece[:, 128:]
        for copy in a_copies(u):
            copy.start()

    def fourier():
        for a in range(4):
            for k1 in range(32):
                fx[k1 * 16 + a * 4 : k1 * 16 + a * 4 + 4, :] = sky_ref[
                    a, :, k1 * 128 : (k1 + 1) * 128
                ]

        def rows_of(i):
            rows = pl.ds(pl.multiple_of(i * 128, 128), 128)
            fz[rows, :] = jnp.dot(
                fx[rows, :], table_ref[...], precision=lax.Precision.HIGHEST,
                preferred_element_type=F32,
            )

        loop(0, 4, rows_of)

        def add(k1, sums):
            re, im = sums
            rows = pl.ds(pl.multiple_of(k1 * 16, 16), 16)
            zr = fz[rows, 0:512]
            zi = fz[rows, 512:1024]
            c = twid_ref[k1, 0:1, :]
            s = twid_ref[k1, 1:2, :]
            return re + (zr * c + zi * s), im + (zi * c - zr * s)

        zero = jnp.zeros((16, 512), F32)
        re, im = lax.fori_loop(0, 32, add, (zero, zero))
        fre[0] = re
        fre[1] = im
        for r in range(4):
            rows = [fre[q, a * 4 + r : a * 4 + r + 1, :] for a in range(4) for q in range(2)]
            fown[r * 8 : r * 8 + 8, :] = jnp.concatenate(rows, axis=0).astype(BF16)

    def f_first():
        return remote(fown, frecv.at[0], f_send.at[0], f_recv.at[0], device(x, y, z, 1 - core))

    def f_copies(part):
        a1, a2, a3, first, _ = pairs(part // 2, part % 2)
        return [
            remote(fown, frecv.at[1 + 2 * part + k], f_send.at[1 + 2 * part + k],
                   f_recv.at[1 + 2 * part + k], at(part // 2, first, a2, a3, core ^ k))
            for k in range(2)
        ]

    def f_start(part):
        for copy in f_copies(part):
            copy.start()

    def build(part):
        axis, par = part // 2, part % 2
        for copy in f_copies(part):
            copy.wait_recv()
        four = jnp.concatenate(
            [fown[...], frecv[0], frecv[1 + 2 * part], frecv[2 + 2 * part]], axis=0
        )
        passed = pl.multiple_of((2 - 2 * par) * 128, 128)
        mine = jnp.concatenate([perm[axis, 384:448, :], perm[axis, pl.ds(passed, 64), :]], axis=0)
        picked = lax.dot_general(
            four, mine, (((1,), (1,)), ((), ())), preferred_element_type=F32
        ).astype(BF16)
        lane = iota((128, 1024), 1)
        spread = (lane >> 7) * 16 + (lane & 15) == iota((128, 1024), 0)
        tiled = jnp.dot(
            picked, jnp.where(spread, 1.0, 0.0).astype(BF16), preferred_element_type=F32
        )
        group = iota((8, 128), 1) >> 4
        diagonal = (iota((128, 128), 0) >> 3) == (iota((128, 128), 1) & 15)
        for g in range(8):
            for h in range(2):
                base = jnp.zeros((8, 128), F32)
                for i in range(8):
                    row = (8 * h + i) * 8
                    base = jnp.where(
                        group == i, tiled[row : row + 8, g * 128 : g * 128 + 128], base
                    )
                full = jnp.concatenate([base] * 16, axis=0)
                amat[part, g, :, h * 128 : h * 128 + 128] = jnp.where(diagonal, full, 0.0).astype(
                    BF16
                )

    def b_copy(u):
        part, axis, par = part_of(u)
        _, a2, a3, _, second = pairs(axis, par)
        return remote(passb.at[u], passr.at[u], b_send.at[u], b_recv.at[u],
                      at(axis, second, a2, a3, core))

    def phase_b(u):
        part, axis, par = part_of(u)
        for copy in a_copies(u):
            copy.wait_recv()
        for g in range(8):
            sub, low = g // 4, 16 * (g % 4)
            slabs = [sendb[u, 0, 2 + sub, r, low : low + 16, :] for r in range(4)]
            for src in range(3):
                slabs += [recvb[u, src, sub, r, low : low + 16, :] for r in range(4)]
            out = jnp.dot(
                amat[part, g], jnp.concatenate(slabs, axis=0), preferred_element_type=F32
            )
            rows = slice((g % 4) * 128, (g % 4) * 128 + 128)
            if sub == 0:
                acc[u, rows, :] = out
            else:
                passb[u, rows, :] = out.astype(BF16)
        b_copy(u).start()

    def c_copies(u):
        part, axis, par = part_of(u)
        a1, a2, a3 = coords(axis)
        return [
            remote(s2.at[u, d], r2.at[u, d], c_send.at[u, d], c_recv.at[u, d],
                   at(axis, a1, (a2 + d + 1) % 4, a3, core))
            for d in range(3)
        ]

    def phase_c(u):
        b_copy(u).wait_recv()
        for d in range(4):
            rows = slice(d * 128, d * 128 + 128)
            total = acc[u, rows, :] + passr[u, rows, :].astype(F32)
            if d == 0:
                acc2[u] = total
            else:
                s2[u, d - 1] = total.astype(BF16)
        for copy in c_copies(u):
            copy.start()

    def d_copies(u):
        part, axis, par = part_of(u)
        a1, a2, a3 = coords(axis)
        return [
            remote(s3.at[u, d], r3.at[u, d], d_send.at[u, d], d_recv.at[u, d],
                   at(axis, a1, a2, (a3 + d + 1) % 4, core))
            for d in range(3)
        ]

    def phase_d(u):
        for copy in c_copies(u):
            copy.wait_recv()
        total = acc2[u]
        for d in range(3):
            total = total + r2[u, d].astype(F32)
        acc3[u] = total[0:32]
        for d in range(3):
            s3[u, d] = total[32 * d + 32 : 32 * d + 64]
        for copy in d_copies(u):
            copy.start()

    column = x * 4 + y
    place = z * 2 + core

    def e_copy(u):
        target = u // 2
        return remote(sp1.at[u], r1s.at[u % 2, place], e_send.at[u], e_recv.at[u % 2, place],
                      device(x, y, target // 2, target % 2))

    def phase_e(u):
        for copy in d_copies(u):
            copy.wait_recv()
        total = acc3[u]
        for d in range(3):
            total = total + r3[u, d]
        ell = (u * LANES + iota((32, 128), 1)).astype(F32)
        total = jnp.where(ell >= morder[...], total, 0.0)
        harm_ref[:, pl.ds(pl.multiple_of(u * LANES, LANES), LANES)] = total
        heavy = total * mweight[...]
        near = [jnp.zeros((8, 128), F32) for _ in range(3)]
        for j in range(4):
            one = total[8 * j : 8 * j + 8]
            weighted = heavy[8 * j : 8 * j + 8]
            for k in range(3):
                other = one if k == 0 else pltpu.roll(one, 8 - 2 * k, 0)
                near[k] = near[k] + weighted * other
        near = [n + pltpu.roll(n, 7, 0) for n in near]
        odd = (iota((8, 128), 0) & 1) == 1
        sp1[u, 0:8, :] = jnp.where(odd, pltpu.roll(near[1], 1, 0), near[0])
        sp1[u, 8:16, :] = near[2]

        @pl.when(u // 2 != place)
        def _():
            e_copy(u).start()

        @pl.when(u // 2 == place)
        def _():
            r1s[u % 2, place] = sp1[u]

    def g_copy(t, k):
        u = 2 * place + t
        return remote(sp2.at[t], r2s.at[column], g_send.at[t, k], g_recv.at[column],
                      device(u // 4, u % 4, k // 2, k % 2))

    def is_me(t, k):
        return jnp.logical_and(2 * place + t == column, k == place)

    def finish():
        for t in range(2):

            def add(k):
                @pl.when(k != place)
                def _():
                    remote(sp1.at[0], r1s.at[t, k], e_send.at[0], e_recv.at[t, k],
                           device(x, y, z, 1 - core)).wait_recv()

            loop(0, 8, add)
            total = r1s[t, 0]
            for k in range(1, 8):
                total = total + r1s[t, k]
            sp2[t] = total

            def send(k):
                @pl.when(jnp.logical_not(is_me(t, k)))
                def _():
                    g_copy(t, k).start()

                @pl.when(is_me(t, k))
                def _():
                    r2s[column] = sp2[t]

            loop(0, 8, send)

        def arrived(k):
            @pl.when(jnp.logical_not(jnp.logical_and(k == column, column // 2 == place)))
            def _():
                remote(sp2.at[0], r2s.at[k], g_send.at[0, 0], g_recv.at[k],
                       device(x, y, z, 1 - core)).wait_recv()

        loop(0, 16, arrived)
        total = r2s[0]
        for k in range(1, 16):
            total = total + r2s[k]
        ell = column * LANES + iota((16, 128), 1)
        total = total / (2 * ell + 1).astype(F32)
        share = ((z % 2) * 2 + core) * 2 + z // 2
        total = pltpu.roll(total, (128 - share * 16) % 128, 1)
        order = [0, 1, 8, 7, 2, 3, 10, 4, 5, 6]
        rows = jnp.concatenate([total[k : k + 1] for k in order], axis=0)
        spec_ref[...] = rows[:, 0:16]

    def orders():
        mine = perm[0, 384:400, :].astype(F32)
        m = jnp.sum(mine * iota((16, 512), 1).astype(F32), axis=1, keepdims=True)
        m = jnp.broadcast_to(m, (16, 128))
        full = jnp.concatenate(
            [jnp.broadcast_to(m[j : j + 1], (8, 128)) for j in range(4)], axis=0
        )
        morder[...] = full
        mweight[...] = jnp.where(full == 0.0, 1.0, 2.0)

    fourier()
    f_first().start()
    loop(0, PARTS, f_start)
    loop(0, 12, phase_a)
    orders()
    f_first().wait_recv()
    loop(0, PARTS, build)
    loop(0, 6, phase_b)
    loop(12, 16, phase_a)
    loop(6, 12, phase_b)
    loop(0, 6, phase_c)
    loop(12, 16, phase_b)
    loop(0, 6, phase_d)
    loop(6, 12, phase_c)
    loop(0, 6, phase_e)
    loop(6, 12, phase_d)
    loop(12, 16, phase_c)
    loop(6, 12, phase_e)
    loop(12, 16, phase_d)
    loop(12, 16, phase_e)
    finish()

    f_first().wait_send()

    def f_left(part):
        for copy in f_copies(part):
            copy.wait_send()

    loop(0, PARTS, f_left)

    def left(u):
        for copy in (*a_copies(u), b_copy(u), *c_copies(u), *d_copies(u)):
            copy.wait_send()

        @pl.when(u // 2 != place)
        def _():
            e_copy(u).wait_send()

    loop(0, UNITS, left)

    def g_left(k):
        for t in range(2):

            @pl.when(jnp.logical_not(is_me(t, k)))
            def _():
                g_copy(t, k).wait_send()

    loop(0, 8, g_left)


def per_device(sky_maps, legendre, owner_table, table, twiddle):
    vmem = pl.BlockSpec(memory_space=pltpu.VMEM)
    dma = pltpu.SemaphoreType.DMA
    V = pltpu.VMEM
    harm, spectra = pl.pallas_call(
        kernel,
        out_shape=(
            jax.ShapeDtypeStruct((32, 2048), F32),
            jax.ShapeDtypeStruct((10, 16), F32),
        ),
        in_specs=[vmem, pl.BlockSpec(memory_space=pl.ANY), vmem, vmem, vmem],
        out_specs=(vmem, vmem),
        scratch_shapes=[
            V((UNITS, 4, 512, 128), BF16),
            V((UNITS, 2, 4, 4, 64, 128), BF16),
            V((UNITS, 3, 2, 4, 64, 128), BF16),
            V((3, 512, 512), BF16),
            V((512, 512), BF16),
            V((PARTS, 8, 128, 256), BF16),
            V((512, 128), F32),
            V((512, 1024), F32),
            V((2, 16, 512), F32),
            V((32, 512), BF16),
            V((13, 32, 512), BF16),
            V((UNITS, 512, 128), F32),
            V((UNITS, 512, 128), BF16),
            V((UNITS, 512, 128), BF16),
            V((UNITS, 128, 128), F32),
            V((UNITS, 3, 128, 128), BF16),
            V((UNITS, 3, 128, 128), BF16),
            V((UNITS, 32, 128), F32),
            V((UNITS, 3, 32, 128), F32),
            V((UNITS, 3, 32, 128), F32),
            V((UNITS, 16, 128), F32),
            V((2, 8, 16, 128), F32),
            V((2, 16, 128), F32),
            V((16, 16, 128), F32),
            V((32, 128), F32),
            V((32, 128), F32),
            dma((UNITS,)),
            dma((UNITS, 3)), dma((UNITS, 3)),
            dma((13,)), dma((13,)),
            dma((UNITS,)), dma((UNITS,)),
            dma((UNITS, 3)), dma((UNITS, 3)),
            dma((UNITS, 3)), dma((UNITS, 3)),
            dma((UNITS,)), dma((2, 8)),
            dma((2, 8)), dma((16,)),
        ],
        compiler_params=pltpu.CompilerParams(
            has_side_effects=True, vmem_limit_bytes=60 * 1024 * 1024
        ),
        name="analysis",
    )(sky_maps, legendre, owner_table.reshape(1, 512), table, twiddle)
    return harm.reshape(4, 4, 2, 2048), spectra


def solution(mesh):
    both = ("blk", "grp")
    inner = jax.shard_map(
        per_device,
        mesh=mesh,
        in_specs=(P(None, both, None), P(both, None, None), P(), P(), P()),
        out_specs=(P(both, None, None, None), P(None, both)),
        check_vma=False,
    )

    def run(sky_maps, legendre, owner_table):
        table, twiddle = dft_tables()
        return inner(sky_maps, legendre, owner_table, jnp.asarray(table), jnp.asarray(twiddle))

    return run
```

```python
import functools
import math

import jax
import jax.numpy as jnp
import numpy as np
from jax import lax
from jax.experimental import pallas as pl
from jax.experimental.pallas import tpu as pltpu
from jax.sharding import PartitionSpec as P

MESH = pl.DeviceIdType.MESH
F32 = jnp.float32
BF16 = jnp.bfloat16
UNITS = 16
PARTS = 6
LANES = 128


def iota(shape, dim):
    return lax.broadcasted_iota(jnp.int32, shape, dim)


def dft_tables():
    k2 = np.arange(128)[:, None]
    m = np.arange(512)[None, :]
    angle = 2.0 * math.pi * ((k2 * m) % 4096) / 4096.0
    table = np.concatenate([np.cos(angle), -np.sin(angle)], axis=1) / 64.0
    k1 = np.arange(32)[:, None]
    turn = 2.0 * math.pi * ((k1 * m) % 32) / 32.0
    twiddle = np.stack([np.cos(turn), np.sin(turn)], axis=1)
    return table.astype(np.float32), twiddle.astype(np.float32)


def kernel(
    sky_in, leg_ref, own_ref, table_in, twid_in, harm_ref, spec_ref,
    sky_ref, table_ref, twid_ref, legv, sendb, recvb, perm, hot, amat, fx, fz, fre, fown, frecv,
    acc, passb, passr, acc2, s2, r2, acc3, s3, r3, sp, rsp, morder, mweight,
    in_sem, leg_sem, a_send, a_recv, f_send, f_recv, b_send, b_recv, c_send, c_recv,
    d_send, d_recv, e_send, e_recv,
):
    blk = lax.axis_index("blk")
    grp = lax.axis_index("grp")
    x = blk // 16
    y = (blk // 4) % 4
    z = grp * 2 + (blk // 2) % 2
    core = blk % 2

    def pick(axis, v0, v1, v2):
        return jnp.where(axis == 0, v0, jnp.where(axis == 1, v1, v2))

    def coords(axis):
        return pick(axis, x, y, z), pick(axis, y, z, x), pick(axis, z, x, y)

    def device(xx, yy, zz, cc):
        return (xx * 16 + yy * 4 + (zz % 2) * 2 + cc, zz // 2)

    def at(axis, v1, v2, v3, cc):
        return device(pick(axis, v1, v3, v2), pick(axis, v2, v1, v3), pick(axis, v3, v2, v1), cc)

    def part_of(u):
        part = u % PARTS
        return part, part // 2, part % 2

    def pairs(axis, par):
        a1, a2, a3 = coords(axis)
        step = (1 - 2 * (a1 % 2)) * (1 - 2 * par)
        first = (a1 + step + 4) % 4
        second = (a1 - step + 4) % 4
        return a1, a2, a3, first, second

    def remote(src, dst, ss, rs, dev):
        return pltpu.make_async_remote_copy(
            src_ref=src, dst_ref=dst, send_sem=ss, recv_sem=rs, device_id=dev, device_id_type=MESH
        )

    def loop(lo, hi, f):
        def body(i, c):
            f(i)
            return c

        lax.fori_loop(lo, hi, body, 0)

    barrier = pltpu.get_barrier_semaphore()
    near_by = [device(x, y, z, 1 - core)]
    for axis in range(3):
        a1, a2, a3 = coords(axis)
        for d in (1, 2, 3):
            near_by.append(at(axis, (a1 + d) % 4, a2, a3, core))
            if d != 2:
                near_by.append(at(axis, (a1 + d) % 4, a2, a3, 1 - core))
    for dev in near_by:
        pl.semaphore_signal(barrier, inc=1, device_id=dev, device_id_type=MESH)

    def leg_copy(u):
        lanes = pl.ds(pl.multiple_of(u * LANES, LANES), LANES)
        return pltpu.make_async_copy(leg_ref.at[:, :, lanes], legv.at[u], leg_sem.at[u])

    inputs = [
        pltpu.make_async_copy(src, dst, in_sem.at[i])
        for i, (src, dst) in enumerate(
            [(sky_in, sky_ref), (table_in, table_ref), (twid_in, twid_ref)]
        )
    ]
    loop(0, PARTS, lambda u: leg_copy(u).start())
    for copy in inputs:
        copy.start()
    loop(PARTS, UNITS, lambda u: leg_copy(u).start())

    def hot_rows(i):
        rows = pl.ds(pl.multiple_of(i * 128, 128), 128)
        same = iota((128, 512), 0) + i * 128 == own_ref[...]
        hot[rows, :] = jnp.where(same, 1.0, 0.0).astype(BF16)

    loop(0, 4, hot_rows)

    def perm_rows(axis):
        a1, a2, a3 = coords(axis)
        step = 1 - 2 * (a1 % 2)
        i = iota((512, 512), 0)
        j = i & 3
        v3 = (a3 + (i >> 2)) & 3
        v2 = (a2 + (i >> 4)) & 3
        cc = core ^ ((i >> 6) & 1)
        v1 = (a1 + ((i >> 7) + 1) * step + 16) & 3
        xx = pick(axis, v1, v3, v2)
        yy = pick(axis, v2, v1, v3)
        zz = pick(axis, v3, v2, v1)
        slot = ((((xx * 4 + yy) * 2 + (zz & 1)) * 2 + cc) * 2 + (zz >> 1)) * 4 + j
        chosen = jnp.where(slot == iota((512, 512), 1), 1.0, 0.0).astype(BF16)
        rows = lax.dot_general(
            chosen, hot[...], (((1,), (1,)), ((), ())), preferred_element_type=F32
        )
        perm[axis] = rows.astype(BF16)

    loop(0, 3, perm_rows)

    def a_copies(u):
        part, axis, par = part_of(u)
        a1, a2, a3, first, _ = pairs(axis, par)
        return (
            remote(sendb.at[u, 1, pl.ds(2, 2)], recvb.at[u, 0], a_send.at[u, 0], a_recv.at[u, 0],
                   at(axis, a1, a2, a3, 1 - core)),
            remote(sendb.at[u, 0, pl.ds(0, 2)], recvb.at[u, 1], a_send.at[u, 1], a_recv.at[u, 1],
                   at(axis, first, a2, a3, core)),
            remote(sendb.at[u, 1, pl.ds(0, 2)], recvb.at[u, 2], a_send.at[u, 2], a_recv.at[u, 2],
                   at(axis, first, a2, a3, 1 - core)),
        )

    def phase_a(u):
        part, axis, par = part_of(u)
        leg_copy(u).wait()
        roles = (3 * par, 1, 3 - 3 * par, 2)
        for pair in range(2):
            wide = jnp.concatenate([legv[u, 2 * pair], legv[u, 2 * pair + 1]], axis=1)
            rows = jnp.dot(perm[axis], wide, preferred_element_type=F32).astype(BF16)
            for rel in range(4):
                for rc in range(2):
                    piece = rows[rel * 128 + rc * 64 : rel * 128 + rc * 64 + 64]
                    sendb[u, rc, roles[rel], 2 * pair] = piece[:, :128]
                    sendb[u, rc, roles[rel], 2 * pair + 1] = piece[:, 128:]
        for copy in a_copies(u):
            copy.start()

    def fourier():
        for copy in inputs:
            copy.wait()
        for a in range(4):
            for k1 in range(32):
                fx[k1 * 16 + a * 4 : k1 * 16 + a * 4 + 4, :] = sky_ref[
                    a, :, k1 * 128 : (k1 + 1) * 128
                ]

        def rows_of(i):
            rows = pl.ds(pl.multiple_of(i * 128, 128), 128)
            fz[rows, :] = jnp.dot(
                fx[rows, :], table_ref[...], precision=lax.Precision.HIGHEST,
                preferred_element_type=F32,
            )

        loop(0, 4, rows_of)

        def add(k1, sums):
            re, im = sums
            rows = pl.ds(pl.multiple_of(k1 * 16, 16), 16)
            zr = fz[rows, 0:512]
            zi = fz[rows, 512:1024]
            c = twid_ref[k1, 0:1, :]
            s = twid_ref[k1, 1:2, :]
            return re + (zr * c + zi * s), im + (zi * c - zr * s)

        zero = jnp.zeros((16, 512), F32)
        re, im = lax.fori_loop(0, 32, add, (zero, zero))
        fre[0] = re
        fre[1] = im
        for r in range(4):
            rows = [fre[q, a * 4 + r : a * 4 + r + 1, :] for a in range(4) for q in range(2)]
            fown[r * 8 : r * 8 + 8, :] = jnp.concatenate(rows, axis=0).astype(BF16)

    def f_first():
        return remote(fown, frecv.at[0], f_send.at[0], f_recv.at[0], device(x, y, z, 1 - core))

    def f_copies(part):
        a1, a2, a3, first, _ = pairs(part // 2, part % 2)
        return [
            remote(fown, frecv.at[1 + 2 * part + k], f_send.at[1 + 2 * part + k],
                   f_recv.at[1 + 2 * part + k], at(part // 2, first, a2, a3, core ^ k))
            for k in range(2)
        ]

    def f_start(part):
        for copy in f_copies(part):
            copy.start()

    def build(part):
        axis, par = part // 2, part % 2
        for copy in f_copies(part):
            copy.wait_recv()
        four = jnp.concatenate(
            [fown[...], frecv[0], frecv[1 + 2 * part], frecv[2 + 2 * part]], axis=0
        )
        passed = pl.multiple_of((2 - 2 * par) * 128, 128)
        mine = jnp.concatenate([perm[axis, 384:448, :], perm[axis, pl.ds(passed, 64), :]], axis=0)
        picked = lax.dot_general(
            four, mine, (((1,), (1,)), ((), ())), preferred_element_type=F32
        ).astype(BF16)
        lane = iota((128, 1024), 1)
        spread = (lane >> 7) * 16 + (lane & 15) == iota((128, 1024), 0)
        tiled = jnp.dot(
            picked, jnp.where(spread, 1.0, 0.0).astype(BF16), preferred_element_type=F32
        )
        group = iota((8, 128), 1) >> 4
        diagonal = (iota((128, 128), 0) >> 3) == (iota((128, 128), 1) & 15)
        for g in range(8):
            for h in range(2):
                base = jnp.zeros((8, 128), F32)
                for i in range(8):
                    row = (8 * h + i) * 8
                    base = jnp.where(
                        group == i, tiled[row : row + 8, g * 128 : g * 128 + 128], base
                    )
                full = jnp.concatenate([base] * 16, axis=0)
                amat[part, g, :, h * 128 : h * 128 + 128] = jnp.where(diagonal, full, 0.0).astype(
                    BF16
                )

    def b_copy(u):
        part, axis, par = part_of(u)
        _, a2, a3, _, second = pairs(axis, par)
        return remote(passb.at[u], passr.at[u], b_send.at[u], b_recv.at[u],
                      at(axis, second, a2, a3, core))

    def phase_b(u):
        part, axis, par = part_of(u)
        for copy in a_copies(u):
            copy.wait_recv()
        for g in range(8):
            sub, low = g // 4, 16 * (g % 4)
            slabs = [sendb[u, 0, 2 + sub, r, low : low + 16, :] for r in range(4)]
            for src in range(3):
                slabs += [recvb[u, src, sub, r, low : low + 16, :] for r in range(4)]
            out = jnp.dot(
                amat[part, g], jnp.concatenate(slabs, axis=0), preferred_element_type=F32
            )
            rows = slice((g % 4) * 128, (g % 4) * 128 + 128)
            if sub == 0:
                acc[u, rows, :] = out
            else:
                passb[u, rows, :] = out.astype(BF16)
        b_copy(u).start()

    def c_copies(u):
        part, axis, par = part_of(u)
        a1, a2, a3 = coords(axis)
        return [
            remote(s2.at[u, d], r2.at[u, d], c_send.at[u, d], c_recv.at[u, d],
                   at(axis, a1, (a2 + d + 1) % 4, a3, core))
            for d in range(3)
        ]

    def phase_c(u):
        b_copy(u).wait_recv()
        for d in range(4):
            rows = slice(d * 128, d * 128 + 128)
            total = acc[u, rows, :] + passr[u, rows, :].astype(F32)
            if d == 0:
                acc2[u] = total
            else:
                s2[u, d - 1] = total.astype(BF16)
        for copy in c_copies(u):
            copy.start()

    def d_copies(u):
        part, axis, par = part_of(u)
        a1, a2, a3 = coords(axis)
        return [
            remote(s3.at[u, d], r3.at[u, d], d_send.at[u, d], d_recv.at[u, d],
                   at(axis, a1, a2, (a3 + d + 1) % 4, core))
            for d in range(3)
        ]

    def phase_d(u):
        for copy in c_copies(u):
            copy.wait_recv()
        total = acc2[u]
        for d in range(3):
            total = total + r2[u, d].astype(F32)
        acc3[u] = total[0:32]
        for d in range(3):
            s3[u, d] = total[32 * d + 32 : 32 * d + 64].astype(BF16)
        for copy in d_copies(u):
            copy.start()

    me = blk * 2 + grp

    def e_copy(u, k):
        slot = (me - (u * 8 + k) + 255) % 128
        return remote(sp.at[u, k], rsp.at[slot], e_send, e_recv, (u * 4 + k // 2, k % 2))

    pair_rows = [(0, 0), (1, 0), (2, 0), (1, 6), (0, 2), (1, 2), (2, 2), (0, 4), (1, 4), (0, 6)]

    def phase_e(u):
        for copy in d_copies(u):
            copy.wait_recv()
        total = acc3[u]
        for d in range(3):
            total = total + r3[u, d].astype(F32)
        ell = (u * LANES + iota((32, 128), 1)).astype(F32)
        total = jnp.where(ell >= morder[...], total, 0.0)
        harm_ref[:, pl.ds(pl.multiple_of(u * LANES, LANES), LANES)] = total
        heavy = total * mweight[...]
        near = [jnp.zeros((8, 128), F32) for _ in range(3)]
        for j in range(4):
            one = total[8 * j : 8 * j + 8]
            weighted = heavy[8 * j : 8 * j + 8]
            for k in range(3):
                other = one if k == 0 else pltpu.roll(one, 8 - 2 * k, 0)
                near[k] = near[k] + weighted * other
        near = [n + pltpu.roll(n, 7, 0) for n in near]
        lane = iota((8, 128), 1) >> 4
        packed = [jnp.zeros((8, 128), F32) for _ in range(2)]
        for p, (k, row) in enumerate(pair_rows):
            moved = near[k] if p % 8 == 0 else pltpu.roll(near[k], 16 * (p % 8), 1)
            wide = jnp.broadcast_to(moved[row : row + 1], (8, 128))
            wide = pltpu.roll(wide, 16, 1, stride=16, stride_axis=0)
            packed[p // 8] = jnp.where(lane == p % 8, wide, packed[p // 8])
        for k in range(8):
            for half in range(2):
                sp[u, k, half : half + 1, :] = packed[half][7 - k : 8 - k]

        def send(k, c):
            @pl.when(u * 8 + k != me)
            def _():
                e_copy(u, k).start()

            return c

        lax.fori_loop(0, 8, send, 0)

    def finish():
        arrived = remote(rsp, rsp, e_send, e_recv, device(x, y, z, 1 - core))
        arrived.wait_recv()
        total = sp[me // 8, me % 8]
        for k in range(127):
            total = total + rsp[k]
        rows = []
        for half in range(2):
            wide = jnp.broadcast_to(total[half : half + 1], (8, 128))
            wide = pltpu.roll(wide, 16, 1, stride=16, stride_axis=0)
            rows += [wide[7 - p : 8 - p, 0:16] for p in range(8)]
        ell = me * 16 + iota((10, 16), 1)
        power = jnp.concatenate(rows[0:10], axis=0)
        spec_ref[...] = power / (2 * ell + 1).astype(F32)
        arrived.wait_send()

    def orders():
        mine = perm[0, 384:400, :].astype(F32)
        m = jnp.sum(mine * iota((16, 512), 1).astype(F32), axis=1, keepdims=True)
        m = jnp.broadcast_to(m, (16, 128))
        full = jnp.concatenate(
            [jnp.broadcast_to(m[j : j + 1], (8, 128)) for j in range(4)], axis=0
        )
        morder[...] = full
        mweight[...] = jnp.where(full == 0.0, 1.0, 2.0)

    def phase(name, lo, hi, f):
        with jax.named_scope(name):
            loop(lo, hi, f)

    with jax.named_scope("meet"):
        pl.semaphore_wait(barrier, len(near_by))
    phase("a0", 0, 6, phase_a)
    with jax.named_scope("fourier"):
        fourier()
        f_first().start()
        loop(0, PARTS, f_start)
        orders()
    phase("a1", 6, 12, phase_a)
    with jax.named_scope("build"):
        f_first().wait_recv()
        loop(0, PARTS, build)
    phase("b0", 0, 6, phase_b)
    phase("a2", 12, 16, phase_a)
    phase("b1", 6, 12, phase_b)
    phase("c0", 0, 6, phase_c)
    phase("b2", 12, 16, phase_b)
    phase("d0", 0, 6, phase_d)
    phase("c1", 6, 12, phase_c)
    phase("e0", 0, 6, phase_e)
    phase("d1", 6, 12, phase_d)
    phase("c2", 12, 16, phase_c)
    phase("e1", 6, 12, phase_e)
    phase("d2", 12, 16, phase_d)
    phase("e2", 12, 16, phase_e)
    with jax.named_scope("finish"):
        finish()

    f_first().wait_send()

    def f_left(part):
        for copy in f_copies(part):
            copy.wait_send()

    loop(0, PARTS, f_left)

    def left(u):
        for copy in (*a_copies(u), b_copy(u), *c_copies(u), *d_copies(u)):
            copy.wait_send()

    with jax.named_scope("left"):
        loop(0, UNITS, left)


def per_device(sky_maps, legendre, owner_table, table, twiddle):
    vmem = pl.BlockSpec(memory_space=pltpu.VMEM)
    away = pl.BlockSpec(memory_space=pl.ANY)
    dma = pltpu.SemaphoreType.DMA
    V = pltpu.VMEM
    harm, spectra = pl.pallas_call(
        kernel,
        out_shape=(
            jax.ShapeDtypeStruct((32, 2048), F32),
            jax.ShapeDtypeStruct((10, 16), F32),
        ),
        in_specs=[away, away, vmem, away, away],
        out_specs=(vmem, vmem),
        scratch_shapes=[
            V((4, 4, 4096), F32),
            V((128, 1024), F32),
            V((32, 2, 512), F32),
            V((UNITS, 4, 512, 128), BF16),
            V((UNITS, 2, 4, 4, 64, 128), BF16),
            V((UNITS, 3, 2, 4, 64, 128), BF16),
            V((3, 512, 512), BF16),
            V((512, 512), BF16),
            V((PARTS, 8, 128, 256), BF16),
            V((512, 128), F32),
            V((512, 1024), F32),
            V((2, 16, 512), F32),
            V((32, 512), BF16),
            V((13, 32, 512), BF16),
            V((UNITS, 512, 128), F32),
            V((UNITS, 512, 128), BF16),
            V((UNITS, 512, 128), BF16),
            V((UNITS, 128, 128), F32),
            V((UNITS, 3, 128, 128), BF16),
            V((UNITS, 3, 128, 128), BF16),
            V((UNITS, 32, 128), F32),
            V((UNITS, 3, 32, 128), BF16),
            V((UNITS, 3, 32, 128), BF16),
            V((UNITS, 8, 2, 128), F32),
            V((127, 2, 128), F32),
            V((32, 128), F32),
            V((32, 128), F32),
            dma((3,)), dma((UNITS,)),
            dma((UNITS, 3)), dma((UNITS, 3)),
            dma((13,)), dma((13,)),
            dma((UNITS,)), dma((UNITS,)),
            dma((UNITS, 3)), dma((UNITS, 3)),
            dma((UNITS, 3)), dma((UNITS, 3)),
            dma, dma,
        ],
        compiler_params=pltpu.CompilerParams(
            collective_id=0, has_side_effects=True, vmem_limit_bytes=60 * 1024 * 1024
        ),
        name="analysis",
    )(sky_maps, legendre, owner_table.reshape(1, 512), table, twiddle)
    return harm.reshape(4, 4, 2, 2048), spectra


def solution(mesh):
    both = ("blk", "grp")
    inner = jax.shard_map(
        per_device,
        mesh=mesh,
        in_specs=(P(None, both, None), P(both, None, None), P(), P(), P()),
        out_specs=(P(both, None, None, None), P(None, both)),
        check_vma=False,
    )

    def run(sky_maps, legendre, owner_table):
        table, twiddle = dft_tables()
        return inner(sky_maps, legendre, owner_table, jnp.asarray(table), jnp.asarray(twiddle))

    return run
```

```python
import functools
import math

import jax
import jax.numpy as jnp
import numpy as np
from jax import lax
from jax.experimental import pallas as pl
from jax.experimental.pallas import tpu as pltpu
from jax.sharding import PartitionSpec as P

MESH = pl.DeviceIdType.MESH
F32 = jnp.float32
BF16 = jnp.bfloat16
UNITS = 16
PARTS = 6
LANES = 128


def iota(shape, dim):
    return lax.broadcasted_iota(jnp.int32, shape, dim)


def dft_tables():
    k2 = np.arange(128)[:, None]
    m = np.arange(512)[None, :]
    angle = 2.0 * math.pi * ((k2 * m) % 4096) / 4096.0
    table = np.concatenate([np.cos(angle), -np.sin(angle)], axis=1) / 64.0
    k1 = np.arange(32)[:, None]
    turn = 2.0 * math.pi * ((k1 * m) % 32) / 32.0
    twiddle = np.stack([np.cos(turn), np.sin(turn)], axis=1)
    table = table.astype(np.float32)
    high = table.astype(jnp.bfloat16)
    low = (table - high.astype(np.float32)).astype(jnp.bfloat16)
    return np.concatenate([high, low], axis=0), twiddle.astype(np.float32)


def kernel(
    sky_in, leg_ref, own_ref, table_in, twid_in, harm_ref, spec_ref,
    sky_ref, table_ref, twid_ref, legv, sendb, recvb, perm, hot, amat, spread, fx, fz, fre, fown, frecv,
    acc, passb, passr, acc2, s2, r2, t2, q2, acc3, s3, r3, harm, sp, rsp, morder, mweight,
    in_sem, leg_sem, out_sem, a_send, a_recv, f_send, f_recv, b_send, b_recv, c_send, c_recv,
    h_send, h_recv, d_send, d_recv, e_send, e_recv,
):
    blk = lax.axis_index("blk")
    grp = lax.axis_index("grp")
    x = blk // 16
    y = (blk // 4) % 4
    z = grp * 2 + (blk // 2) % 2
    core = blk % 2

    def pick(axis, v0, v1, v2):
        return jnp.where(axis == 0, v0, jnp.where(axis == 1, v1, v2))

    def coords(axis):
        return pick(axis, x, y, z), pick(axis, y, z, x), pick(axis, z, x, y)

    def device(xx, yy, zz, cc):
        return (xx * 16 + yy * 4 + (zz % 2) * 2 + cc, zz // 2)

    def at(axis, v1, v2, v3, cc):
        return device(pick(axis, v1, v3, v2), pick(axis, v2, v1, v3), pick(axis, v3, v2, v1), cc)

    def part_of(u):
        part = u % PARTS
        return part, part // 2, part % 2

    def pairs(axis, par):
        a1, a2, a3 = coords(axis)
        step = (1 - 2 * (a1 % 2)) * (1 - 2 * par)
        first = (a1 + step + 4) % 4
        second = (a1 - step + 4) % 4
        return a1, a2, a3, first, second

    def remote(src, dst, ss, rs, dev):
        return pltpu.make_async_remote_copy(
            src_ref=src, dst_ref=dst, send_sem=ss, recv_sem=rs, device_id=dev, device_id_type=MESH
        )

    def loop(lo, hi, f):
        def body(i, c):
            f(i)
            return c

        lax.fori_loop(lo, hi, body, 0)

    barrier = pltpu.get_barrier_semaphore()
    near_by = [device(x, y, z, 1 - core)]
    for axis in range(3):
        a1, a2, a3 = coords(axis)
        for d in (1, 2, 3):
            near_by.append(at(axis, (a1 + d) % 4, a2, a3, core))
            if d != 2:
                near_by.append(at(axis, (a1 + d) % 4, a2, a3, 1 - core))
    for dev in near_by:
        pl.semaphore_signal(barrier, inc=1, device_id=dev, device_id_type=MESH)

    def leg_copy(u):
        lanes = pl.ds(pl.multiple_of(u * LANES, LANES), LANES)
        return pltpu.make_async_copy(leg_ref.at[:, :, lanes], legv.at[u], leg_sem.at[u])

    inputs = [
        pltpu.make_async_copy(src, dst, in_sem.at[i])
        for i, (src, dst) in enumerate(
            [(sky_in, sky_ref), (table_in, table_ref), (twid_in, twid_ref)]
        )
    ]
    loop(0, PARTS, lambda u: leg_copy(u).start())
    for copy in inputs:
        copy.start()
    loop(PARTS, UNITS, lambda u: leg_copy(u).start())

    def hot_rows(i):
        rows = pl.ds(pl.multiple_of(i * 128, 128), 128)
        same = iota((128, 512), 0) + i * 128 == own_ref[...]
        hot[rows, :] = jnp.where(same, 1.0, 0.0).astype(BF16)

    loop(0, 4, hot_rows)

    def perm_rows(axis):
        a1, a2, a3 = coords(axis)
        i = iota((512, 128), 0)
        v3 = (a3 + (i >> 2)) & 3
        v2 = (a2 + ((i >> 4) + 1) * (1 - 2 * (a2 % 2)) + 128) & 3
        v1 = (a1 + ((i >> 7) + 1) * (1 - 2 * (a1 % 2)) + 16) & 3
        cc = core ^ ((i >> 6) & 1)
        xx, yy, zz = ((v1, v2, v3), (v3, v1, v2), (v2, v3, v1))[axis]
        slot = (xx << 7) + (yy << 5) + ((zz & 1) << 4) + (cc << 3) + ((zz >> 1) << 2) + (i & 3)
        slot = slot - iota((512, 128), 1)
        chosen = jnp.concatenate(
            [jnp.where(slot == k * 128, 1.0, 0.0).astype(BF16) for k in range(4)], axis=1
        )
        rows = lax.dot_general(
            chosen, hot[...], (((1,), (1,)), ((), ())), preferred_element_type=F32
        )
        perm[axis] = rows.astype(BF16)

    def a_copies(u):
        part, axis, par = part_of(u)
        a1, a2, a3, first, _ = pairs(axis, par)
        sem = a_recv.at[u]
        return (
            remote(sendb.at[u, 0, pl.ds(0, 2)], recvb.at[u, 1], a_send, sem,
                   at(axis, first, a2, a3, core)),
            remote(sendb.at[u, 1, pl.ds(0, 2)], recvb.at[u, 2], a_send, sem,
                   at(axis, first, a2, a3, 1 - core)),
            remote(sendb.at[u, 1, pl.ds(2, 2)], recvb.at[u, 0], a_send, sem,
                   at(axis, a1, a2, a3, 1 - core)),
        )

    def a_rows(u):
        part, axis, par = part_of(u)
        leg_copy(u).wait()
        roles = (3 * par, 1, 3 - 3 * par, 2)
        for pair in range(2):
            wide = jnp.concatenate([legv[u, 2 * pair], legv[u, 2 * pair + 1]], axis=1)
            rows = jnp.dot(perm[axis], wide, preferred_element_type=F32).astype(BF16)
            for rel in range(4):
                for rc in range(2):
                    piece = rows[rel * 128 + rc * 64 : rel * 128 + rc * 64 + 64]
                    sendb[u, rc, roles[rel], 2 * pair] = piece[:, :128]
                    sendb[u, rc, roles[rel], 2 * pair + 1] = piece[:, 128:]

    def a_start(u):
        for copy in a_copies(u):
            copy.start()

    def phase_a(u):
        a_rows(u)
        a_start(u)

    def all_in(ref, sem):
        remote(ref, ref, a_send, sem, device(x, y, z, 1 - core)).wait_recv()

    def all_out(ref, sem):
        remote(ref, ref, sem, e_recv, device(x, y, z, 1 - core)).wait_send()

    def fourier():
        for copy in inputs:
            copy.wait()
        for a in range(4):
            for k1 in range(32):
                fx[k1 * 16 + a * 4 : k1 * 16 + a * 4 + 4, :] = sky_ref[
                    a, :, k1 * 128 : (k1 + 1) * 128
                ]

        def rows_of(i):
            rows = pl.ds(pl.multiple_of(i * 128, 128), 128)
            pixels = fx[rows, :]
            high = pixels.astype(BF16)
            low = (pixels - high.astype(F32)).astype(BF16)
            table = table_ref[0:128, :]
            fz[rows, :] = jnp.dot(
                jnp.concatenate([high, low], axis=1), jnp.concatenate([table, table], axis=0),
                preferred_element_type=F32,
            ) + jnp.dot(high, table_ref[128:256, :], preferred_element_type=F32)

        loop(0, 4, rows_of)

        def add(k1, sums):
            re, im = sums
            rows = pl.ds(pl.multiple_of(k1 * 16, 16), 16)
            zr = fz[rows, 0:512]
            zi = fz[rows, 512:1024]
            c = twid_ref[k1, 0:1, :]
            s = twid_ref[k1, 1:2, :]
            return re + (zr * c + zi * s), im + (zi * c - zr * s)

        zero = jnp.zeros((16, 512), F32)
        re, im = lax.fori_loop(0, 32, add, (zero, zero))
        fre[0] = re
        fre[1] = im
        for r in range(4):
            rows = [fre[q, a * 4 + r : a * 4 + r + 1, :] for a in range(4) for q in range(2)]
            fown[r * 8 : r * 8 + 8, :] = jnp.concatenate(rows, axis=0).astype(BF16)

    def f_first():
        return remote(fown, frecv.at[0], f_send, f_recv.at[6], device(x, y, z, 1 - core))

    def f_copies(part):
        a1, a2, a3, first, _ = pairs(part // 2, part % 2)
        return [
            remote(fown, frecv.at[1 + 2 * part + k], f_send, f_recv.at[part],
                   at(part // 2, first, a2, a3, core ^ k))
            for k in range(2)
        ]

    def f_start(part):
        for copy in f_copies(part):
            copy.start()

    def build(part):
        axis, par = part // 2, part % 2
        four = jnp.concatenate(
            [fown[...], frecv[0], frecv[1 + 2 * part], frecv[2 + 2 * part]], axis=0
        )
        passed = pl.multiple_of((2 - 2 * par) * 128, 128)
        mine = jnp.concatenate([perm[axis, 384:448, :], perm[axis, pl.ds(passed, 64), :]], axis=0)
        picked = lax.dot_general(
            four, mine, (((1,), (1,)), ((), ())), preferred_element_type=F32
        ).astype(BF16)
        tiled = jnp.dot(
            picked, spread[...], preferred_element_type=F32
        )
        group = iota((8, 128), 1) >> 4
        diagonal = (iota((128, 128), 0) >> 3) == (iota((128, 128), 1) & 15)
        for g in range(8):
            for h in range(2):
                base = jnp.zeros((8, 128), F32)
                for i in range(8):
                    row = (8 * h + i) * 8
                    base = jnp.where(
                        group == i, tiled[row : row + 8, g * 128 : g * 128 + 128], base
                    )
                full = jnp.concatenate([base] * 16, axis=0)
                amat[part, g, :, h * 128 : h * 128 + 128] = jnp.where(diagonal, full, 0.0).astype(
                    BF16
                )

    def b_copy(u):
        part, axis, par = part_of(u)
        _, a2, a3, _, second = pairs(axis, par)
        return remote(passb.at[u], passr.at[u], b_send, b_recv.at[u],
                      at(axis, second, a2, a3, core))

    def phase_b(u):
        part, axis, par = part_of(u)
        all_in(recvb.at[u], a_recv.at[u])
        for g in range(8):
            sub, low = g // 4, 16 * (g % 4)
            slabs = [sendb[u, 0, 2 + sub, r, low : low + 16, :] for r in range(4)]
            for src in range(3):
                slabs += [recvb[u, src, sub, r, low : low + 16, :] for r in range(4)]
            out = jnp.dot(
                amat[part, g], jnp.concatenate(slabs, axis=0), preferred_element_type=F32
            )
            rows = slice((g % 4) * 128, (g % 4) * 128 + 128)
            if sub == 0:
                acc[u, rows, :] = out
            else:
                passb[u, rows, :] = out.astype(BF16)
        b_copy(u).start()

    def second_pairs(axis, par):
        a1, a2, a3 = coords(axis)
        step = (1 - 2 * (a2 % 2)) * (1 - 2 * par)
        return (at(axis, a1, (a2 + step + 4) % 4, a3, core),
                at(axis, a1, (a2 - step + 4) % 4, a3, core))

    def c_copy(u):
        part, axis, par = part_of(u)
        return remote(s2.at[u], r2.at[u], c_send, c_recv.at[u], second_pairs(axis, par)[0])

    def phase_c(u):
        part, axis, par = part_of(u)
        all_in(passr.at[u], b_recv.at[u])

        def total(rel):
            rows = pl.ds(pl.multiple_of(rel * 128, 128), 128)
            return acc[u, rows, :] + passr[u, rows, :].astype(F32)

        s2[u, 0] = total(2 * par).astype(BF16)
        s2[u, 1] = total(1).astype(BF16)
        c_copy(u).start()
        acc2[u, 0] = total(3)
        acc2[u, 1] = total(2 - 2 * par)

    def h_copy(u):
        part, axis, par = part_of(u)
        return remote(t2.at[u], q2.at[u], h_send, h_recv.at[u], second_pairs(axis, par)[1])

    def phase_h(u):
        all_in(r2.at[u], c_recv.at[u])
        t2[u] = (acc2[u, 1] + r2[u, 1].astype(F32)).astype(BF16)
        h_copy(u).start()
        acc2[u, 0] = acc2[u, 0] + r2[u, 0].astype(F32)

    def d_copies(u):
        part, axis, par = part_of(u)
        a1, a2, a3 = coords(axis)
        return [
            remote(s3.at[u, d], r3.at[u, d], d_send, d_recv.at[u],
                   at(axis, a1, a2, (a3 + d + 1) % 4, core))
            for d in range(3)
        ]

    def phase_d(u):
        all_in(q2.at[u], h_recv.at[u])
        total = acc2[u, 0] + q2[u].astype(F32)
        for d in range(3):
            s3[u, d] = total[32 * d + 32 : 32 * d + 64].astype(BF16)
        for copy in d_copies(u):
            copy.start()
        acc3[u] = total[0:32]

    me = blk * 2 + grp

    def e_copy(u, k):
        slot = (me - (u * 8 + k) + 255) % 128
        return remote(sp.at[u, k], rsp.at[slot], e_send, e_recv, (u * 4 + k // 2, k % 2))

    pair_rows = [(0, 0), (1, 0), (2, 0), (1, 6), (0, 2), (1, 2), (2, 2), (0, 4), (1, 4), (0, 6)]

    def phase_e(u):
        all_in(r3.at[u], d_recv.at[u])
        total = acc3[u]
        for d in range(3):
            total = total + r3[u, d].astype(F32)
        ell = (u * LANES + iota((32, 128), 1)).astype(F32)
        total = jnp.where(ell >= morder[...], total, 0.0)
        lanes = pl.ds(pl.multiple_of(u * LANES, LANES), LANES)
        harm[:, lanes] = total
        pltpu.make_async_copy(harm.at[:, lanes], harm_ref.at[:, lanes], out_sem).start()
        heavy = total * mweight[...]
        near = [jnp.zeros((8, 128), F32) for _ in range(3)]
        for j in range(4):
            one = total[8 * j : 8 * j + 8]
            weighted = heavy[8 * j : 8 * j + 8]
            for k in range(3):
                other = one if k == 0 else pltpu.roll(one, 8 - 2 * k, 0)
                near[k] = near[k] + weighted * other
        near = [n + pltpu.roll(n, 7, 0) for n in near]
        lane = iota((8, 128), 1) >> 4
        packed = [jnp.zeros((8, 128), F32) for _ in range(2)]
        for p, (k, row) in enumerate(pair_rows):
            moved = near[k] if p % 8 == 0 else pltpu.roll(near[k], 16 * (p % 8), 1)
            wide = jnp.broadcast_to(moved[row : row + 1], (8, 128))
            wide = pltpu.roll(wide, 16, 1, stride=16, stride_axis=0)
            packed[p // 8] = jnp.where(lane == p % 8, wide, packed[p // 8])
        for k in range(8):
            for half in range(2):
                sp[u, k, half : half + 1, :] = packed[half][7 - k : 8 - k]

        for k in range(8):

            @pl.when(u * 8 + k != me)
            def _():
                e_copy(u, k).start()

    def finish():
        arrived = remote(rsp, rsp, e_send, e_recv, device(x, y, z, 1 - core))
        arrived.wait_recv()
        total = sp[me // 8, me % 8]
        for k in range(127):
            total = total + rsp[k]
        rows = []
        for half in range(2):
            wide = jnp.broadcast_to(total[half : half + 1], (8, 128))
            wide = pltpu.roll(wide, 16, 1, stride=16, stride_axis=0)
            rows += [wide[7 - p : 8 - p, 0:16] for p in range(8)]
        ell = me * 16 + iota((10, 16), 1)
        power = jnp.concatenate(rows[0:10], axis=0)
        spec_ref[...] = power / (2 * ell + 1).astype(F32)
        arrived.wait_send()
        pltpu.make_async_copy(harm, harm_ref, out_sem).wait()

    def orders():
        mine = perm[0, 432:448, :].astype(F32)
        m = jnp.sum(mine * iota((16, 512), 1).astype(F32), axis=1, keepdims=True)
        m = jnp.broadcast_to(m, (16, 128))
        full = jnp.concatenate(
            [jnp.broadcast_to(m[j : j + 1], (8, 128)) for j in range(4)], axis=0
        )
        morder[...] = full
        mweight[...] = jnp.where(full == 0.0, 1.0, 2.0)

    def phase(name, lo, hi, f):
        with jax.named_scope(name):
            loop(lo, hi, f)

    with jax.named_scope("a0"):
        perm_rows(0)
        a_rows(0)
        with jax.named_scope("meet"):
            pl.semaphore_wait(barrier, len(near_by))
        a_start(0)
        perm_rows(1)
        phase_a(2)
        phase_a(1)
        phase_a(3)
        perm_rows(2)
        loop(4, 6, phase_a)
    with jax.named_scope("fourier"):
        fourier()
        f_first().start()
        loop(0, PARTS, f_start)
    phase("a1", 6, 12, phase_a)
    phase("a2", 12, 16, phase_a)
    with jax.named_scope("build"):
        orders()
        lane = iota((128, 1024), 1)
        same = (lane >> 7) * 16 + (lane & 15) == iota((128, 1024), 0)
        spread[...] = jnp.where(same, 1.0, 0.0).astype(BF16)
        all_in(frecv.at[0], f_recv.at[6])
        for part in range(PARTS):
            all_in(frecv.at[pl.ds(1 + 2 * part, 2)], f_recv.at[part])
        for part in range(PARTS):
            build(part)
    phase("b0", 0, 6, phase_b)
    phase("b1", 6, 12, phase_b)
    phase("b2", 12, 16, phase_b)
    phase("c0", 0, 6, phase_c)
    phase("c1", 6, 12, phase_c)
    phase("c2", 12, 16, phase_c)
    phase("h0", 0, 6, phase_h)
    phase("h1", 6, 12, phase_h)
    phase("h2", 12, 16, phase_h)
    phase("d0", 0, 6, phase_d)
    phase("d1", 6, 12, phase_d)
    phase("d2", 12, 16, phase_d)
    phase("e0", 0, 6, phase_e)
    phase("e1", 6, 12, phase_e)
    phase("e2", 12, 16, phase_e)
    with jax.named_scope("finish"):
        finish()

    with jax.named_scope("left"):
        all_out(frecv, f_send)
        all_out(recvb, a_send)
        all_out(passb, b_send)
        all_out(s2, c_send)
        all_out(t2, h_send)
        all_out(s3, d_send)


def per_device(sky_maps, legendre, owner_table, table, twiddle):
    vmem = pl.BlockSpec(memory_space=pltpu.VMEM)
    away = pl.BlockSpec(memory_space=pl.ANY)
    dma = pltpu.SemaphoreType.DMA
    V = pltpu.VMEM
    harm, spectra = pl.pallas_call(
        kernel,
        out_shape=(
            jax.ShapeDtypeStruct((32, 2048), F32),
            jax.ShapeDtypeStruct((10, 16), F32),
        ),
        in_specs=[away, away, vmem, away, away],
        out_specs=(away, vmem),
        scratch_shapes=[
            V((4, 4, 4096), F32),
            V((256, 1024), BF16),
            V((32, 2, 512), F32),
            V((UNITS, 4, 512, 128), BF16),
            V((UNITS, 2, 4, 4, 64, 128), BF16),
            V((UNITS, 3, 2, 4, 64, 128), BF16),
            V((3, 512, 512), BF16),
            V((512, 512), BF16),
            V((PARTS, 8, 128, 256), BF16),
            V((128, 1024), BF16),
            V((512, 128), F32),
            V((512, 1024), F32),
            V((2, 16, 512), F32),
            V((32, 512), BF16),
            V((13, 32, 512), BF16),
            V((UNITS, 512, 128), F32),
            V((UNITS, 512, 128), BF16),
            V((UNITS, 512, 128), BF16),
            V((UNITS, 2, 128, 128), F32),
            V((UNITS, 2, 128, 128), BF16),
            V((UNITS, 2, 128, 128), BF16),
            V((UNITS, 128, 128), BF16),
            V((UNITS, 128, 128), BF16),
            V((UNITS, 32, 128), F32),
            V((UNITS, 3, 32, 128), BF16),
            V((UNITS, 3, 32, 128), BF16),
            V((32, 2048), F32),
            V((UNITS, 8, 2, 128), F32),
            V((127, 2, 128), F32),
            V((32, 128), F32),
            V((32, 128), F32),
            dma((3,)), dma((UNITS,)), dma,
            dma, dma((UNITS,)), dma, dma((7,)),
            dma, dma((UNITS,)), dma, dma((UNITS,)), dma, dma((UNITS,)), dma, dma((UNITS,)),
            dma, dma,
        ],
        compiler_params=pltpu.CompilerParams(
            collective_id=0, has_side_effects=True, vmem_limit_bytes=60 * 1024 * 1024
        ),
        name="analysis",
    )(sky_maps, legendre, owner_table.reshape(1, 512), table, twiddle)
    return harm.reshape(4, 4, 2, 2048), spectra


def solution(mesh):
    both = ("blk", "grp")
    inner = jax.shard_map(
        per_device,
        mesh=mesh,
        in_specs=(P(None, both, None), P(both, None, None), P(), P(), P()),
        out_specs=(P(both, None, None, None), P(None, both)),
        check_vma=False,
    )

    def run(sky_maps, legendre, owner_table):
        table, twiddle = dft_tables()
        return inner(sky_maps, legendre, owner_table, jnp.asarray(table), jnp.asarray(twiddle))

    return run
```

```python
import functools
import math

import jax
import jax.numpy as jnp
import numpy as np
from jax import lax
from jax.experimental import pallas as pl
from jax.experimental.pallas import tpu as pltpu
from jax.sharding import PartitionSpec as P

MESH = pl.DeviceIdType.MESH
F32 = jnp.float32
BF16 = jnp.bfloat16
UNITS = 16
PARTS = 6
LANES = 128


def iota(shape, dim):
    return lax.broadcasted_iota(jnp.int32, shape, dim)


def dft_tables():
    k2 = np.arange(128)[:, None]
    m = np.arange(512)[None, :]
    angle = 2.0 * math.pi * ((k2 * m) % 4096) / 4096.0
    table = np.concatenate([np.cos(angle), -np.sin(angle)], axis=1) / 64.0
    k1 = np.arange(32)[:, None]
    turn = 2.0 * math.pi * ((k1 * m) % 32) / 32.0
    twiddle = np.stack([np.cos(turn), np.sin(turn)], axis=1)
    table = table.astype(np.float32)
    high = table.astype(jnp.bfloat16)
    low = (table - high.astype(np.float32)).astype(jnp.bfloat16)
    lane = np.arange(1024)[None, :]
    spread = (lane >> 7) * 16 + (lane & 15) == np.arange(128)[:, None]
    diagonal = (np.arange(128)[:, None] >> 3) == (np.arange(128)[None, :] & 15)
    small = np.concatenate([spread, np.tile(diagonal, (1, 8))], axis=0).astype(jnp.bfloat16)
    return np.concatenate([high, low, small], axis=0), twiddle.astype(np.float32)


def kernel(
    sky_in, leg_ref, own_in, table_in, twid_in, harm_ref, spec_ref,
    sky_ref, own_ref, table_ref, twid_ref, legv, sendb, recvb, perm, hot, amat, fx, fz, fre, fown, fkeep, fsend, frecv,
    acc, passb, passr, acc2, s2, r2, t2, q2, acc3, s3, r3, sp, rsp, morder, mweight,
    in_sem, leg_sem, a_send, a_recv, f_send, f_recv, b_send, b_recv, c_send, c_recv,
    h_send, h_recv, d_send, d_recv, e_send, e_recv,
):
    blk = lax.axis_index("blk")
    grp = lax.axis_index("grp")
    x = blk // 16
    y = (blk // 4) % 4
    z = grp * 2 + (blk // 2) % 2
    core = blk % 2

    def pick(axis, v0, v1, v2):
        return jnp.where(axis == 0, v0, jnp.where(axis == 1, v1, v2))

    def coords(axis):
        return pick(axis, x, y, z), pick(axis, y, z, x), pick(axis, z, x, y)

    def device(xx, yy, zz, cc):
        return (xx * 16 + yy * 4 + (zz % 2) * 2 + cc, zz // 2)

    def at(axis, v1, v2, v3, cc):
        return device(pick(axis, v1, v3, v2), pick(axis, v2, v1, v3), pick(axis, v3, v2, v1), cc)

    def part_of(u):
        part = u % PARTS
        return part, part // 2, part % 2

    def pairs(axis, par):
        a1, a2, a3 = coords(axis)
        step = (1 - 2 * (a1 % 2)) * (1 - 2 * par)
        first = (a1 + step + 4) % 4
        second = (a1 - step + 4) % 4
        return a1, a2, a3, first, second

    def remote(src, dst, ss, rs, dev):
        return pltpu.make_async_remote_copy(
            src_ref=src, dst_ref=dst, send_sem=ss, recv_sem=rs, device_id=dev, device_id_type=MESH
        )

    def loop(lo, hi, f):
        def body(i, c):
            f(i)
            return c

        lax.fori_loop(lo, hi, body, 0)

    barrier = pltpu.get_barrier_semaphore()
    near_by = [device(x, y, z, 1 - core)]
    for axis in range(3):
        a1, a2, a3 = coords(axis)
        for d in (1, 2, 3):
            near_by.append(at(axis, (a1 + d) % 4, a2, a3, core))
            if d != 2:
                near_by.append(at(axis, (a1 + d) % 4, a2, a3, 1 - core))
    for dev in near_by:
        pl.semaphore_signal(barrier, inc=1, device_id=dev, device_id_type=MESH)

    def leg_copy(u):
        lanes = pl.ds(pl.multiple_of(u * LANES, LANES), LANES)
        return pltpu.make_async_copy(leg_ref.at[:, :, lanes], legv.at[u], leg_sem.at[u])

    inputs = [
        pltpu.make_async_copy(src, dst, in_sem.at[i])
        for i, (src, dst) in enumerate(
            [(own_in, own_ref), (sky_in, sky_ref), (table_in, table_ref), (twid_in, twid_ref)]
        )
    ]
    inputs[0].start()
    loop(0, PARTS, lambda u: leg_copy(u).start())
    for copy in inputs[1:]:
        copy.start()
    loop(PARTS, UNITS, lambda u: leg_copy(u).start())
    inputs[0].wait()

    def hot_rows(i):
        rows = pl.ds(pl.multiple_of(i * 128, 128), 128)
        same = iota((128, 512), 0) + i * 128 == own_ref[...]
        hot[rows, :] = jnp.where(same, 1.0, 0.0).astype(BF16)

    loop(0, 4, hot_rows)

    def perm_rows(axis):
        a1, a2, a3 = coords(axis)
        i = iota((512, 128), 0)
        v3 = (a3 + ((i >> 2) + 1) * (1 - 2 * (a3 % 2)) + 512) & 3
        v2 = (a2 + ((i >> 4) + 1) * (1 - 2 * (a2 % 2)) + 128) & 3
        v1 = (a1 + ((i >> 7) + 1) * (1 - 2 * (a1 % 2)) + 16) & 3
        cc = core ^ ((i >> 6) & 1)
        xx, yy, zz = ((v1, v2, v3), (v3, v1, v2), (v2, v3, v1))[axis]
        slot = (xx << 7) + (yy << 5) + ((zz & 1) << 4) + (cc << 3) + ((zz >> 1) << 2) + (i & 3)
        slot = slot - iota((512, 128), 1)
        chosen = jnp.concatenate(
            [jnp.where(slot == k * 128, 1.0, 0.0).astype(BF16) for k in range(4)], axis=1
        )
        rows = lax.dot_general(
            chosen, hot[...], (((1,), (1,)), ((), ())), preferred_element_type=F32
        )
        perm[axis] = rows.astype(BF16)

    def a_copies(u):
        part, axis, par = part_of(u)
        a1, a2, a3, first, _ = pairs(axis, par)
        sem = a_recv.at[u]
        return (
            remote(sendb.at[u, 0, pl.ds(0, 2)], recvb.at[u, 1], a_send, sem,
                   at(axis, first, a2, a3, core)),
            remote(sendb.at[u, 1, pl.ds(0, 2)], recvb.at[u, 2], a_send, sem,
                   at(axis, first, a2, a3, 1 - core)),
            remote(sendb.at[u, 1, pl.ds(2, 2)], recvb.at[u, 0], a_send, sem,
                   at(axis, a1, a2, a3, 1 - core)),
        )

    def a_rows(u):
        part, axis, par = part_of(u)
        leg_copy(u).wait()
        roles = (3 * par, 1, 3 - 3 * par, 2)
        for pair in range(2):
            wide = jnp.concatenate([legv[u, 2 * pair], legv[u, 2 * pair + 1]], axis=1)
            rows = jnp.dot(perm[axis], wide, preferred_element_type=F32).astype(BF16)
            for rel in range(4):
                for rc in range(2):
                    piece = rows[rel * 128 + rc * 64 : rel * 128 + rc * 64 + 64]
                    sendb[u, rc, roles[rel], 2 * pair] = piece[:, :128]
                    sendb[u, rc, roles[rel], 2 * pair + 1] = piece[:, 128:]

    def a_start(u):
        for copy in a_copies(u):
            copy.start()

    def phase_a(u):
        a_rows(u)
        a_start(u)

    def all_in(ref, sem):
        remote(ref, ref, a_send, sem, device(x, y, z, 1 - core)).wait_recv()

    def all_out(ref, sem):
        remote(ref, ref, sem, e_recv, device(x, y, z, 1 - core)).wait_send()

    def fourier():
        for copy in inputs[1:]:
            copy.wait()
        for a in range(4):
            for k1 in range(32):
                fx[k1 * 16 + a * 4 : k1 * 16 + a * 4 + 4, :] = sky_ref[
                    a, :, k1 * 128 : (k1 + 1) * 128
                ]

        def rows_of(i):
            rows = pl.ds(pl.multiple_of(i * 128, 128), 128)
            pixels = fx[rows, :]
            high = pixels.astype(BF16)
            low = (pixels - high.astype(F32)).astype(BF16)
            table = table_ref[0:128, :]
            fz[rows, :] = jnp.dot(
                jnp.concatenate([high, low], axis=1), jnp.concatenate([table, table], axis=0),
                preferred_element_type=F32,
            ) + jnp.dot(high, table_ref[128:256, :], preferred_element_type=F32)

        loop(0, 4, rows_of)

        def add(k1, sums):
            re, im = sums
            rows = pl.ds(pl.multiple_of(k1 * 16, 16), 16)
            zr = fz[rows, 0:512]
            zi = fz[rows, 512:1024]
            c = twid_ref[k1, 0:1, :]
            s = twid_ref[k1, 1:2, :]
            return re + (zr * c + zi * s), im + (zi * c - zr * s)

        zero = jnp.zeros((16, 512), F32)
        re, im = lax.fori_loop(0, 32, add, (zero, zero))
        fre[0] = re
        fre[1] = im
        for r in range(4):
            rows = [fre[q, a * 4 + r : a * 4 + r + 1, :] for a in range(4) for q in range(2)]
            fown[r * 8 : r * 8 + 8, :] = jnp.concatenate(rows, axis=0).astype(BF16)

    def f_copies(part):
        axis, par = part // 2, part % 2
        a1, a2, a3, first, _ = pairs(axis, par)
        sem = f_recv.at[part]
        return (
            remote(fsend.at[part, 0], frecv.at[part, 1], f_send, sem, at(axis, first, a2, a3, core)),
            remote(fsend.at[part, 1], frecv.at[part, 2], f_send, sem,
                   at(axis, first, a2, a3, 1 - core)),
            remote(fsend.at[part, 2], frecv.at[part, 0], f_send, sem,
                   at(axis, a1, a2, a3, 1 - core)),
        )

    def f_start():
        low = iota((32, 128), 1) < 64
        for axis in range(3):
            cols = lax.dot_general(
                fown[...], perm[axis], (((1,), (1,)), ((), ())), preferred_element_type=F32
            )
            tile = [cols[:, k * 128 : k * 128 + 128] for k in range(4)]
            turned = [pltpu.roll(t, 64, 1) for t in tile]

            def joined(mine, passed, rc):
                if rc == 0:
                    return jnp.where(low, tile[mine], turned[passed]).astype(BF16)
                return jnp.where(low, turned[mine], tile[passed]).astype(BF16)

            for par in range(2):
                part = 2 * axis + par
                fsend[part, 0] = joined(2 * par, 1, 0)
                fsend[part, 1] = joined(2 * par, 1, 1)
                fsend[part, 2] = joined(3, 2 - 2 * par, 1)
                fkeep[part] = joined(3, 2 - 2 * par, 0)
                for copy in f_copies(part):
                    copy.start()

    def build(part):
        all_in(frecv.at[part], f_recv.at[part])
        picked = jnp.concatenate([fkeep[part]] + [frecv[part, k] for k in range(3)], axis=0)
        tiled = jnp.dot(picked, table_ref[256:384, :], preferred_element_type=F32)
        group = iota((8, 128), 1) >> 4
        for g in range(8):
            for h in range(2):
                base = tiled[64 * h : 64 * h + 8, g * 128 : g * 128 + 128]
                for i in range(1, 8):
                    row = (8 * h + i) * 8
                    base = jnp.where(
                        group == i, tiled[row : row + 8, g * 128 : g * 128 + 128], base
                    )
                two = jnp.concatenate([base, base], axis=0).astype(BF16)
                for k in range(8):
                    rows = slice(16 * k, 16 * k + 16)
                    amat[part, g, rows, h * 128 : h * 128 + 128] = (
                        two * table_ref[384 + 16 * k : 400 + 16 * k, 0:128]
                    )

    def b_copy(u):
        part, axis, par = part_of(u)
        _, a2, a3, _, second = pairs(axis, par)
        return remote(passb.at[u], passr.at[u], b_send, b_recv.at[u],
                      at(axis, second, a2, a3, core))

    def phase_b(u):
        part, axis, par = part_of(u)
        all_in(recvb.at[u], a_recv.at[u])
        for g in range(8):
            sub, low = g // 4, 16 * (g % 4)
            slabs = [sendb[u, 0, 2 + sub, r, low : low + 16, :] for r in range(4)]
            for src in range(3):
                slabs += [recvb[u, src, sub, r, low : low + 16, :] for r in range(4)]
            out = jnp.dot(
                amat[part, g], jnp.concatenate(slabs, axis=0), preferred_element_type=F32
            )
            rows = slice((g % 4) * 128, (g % 4) * 128 + 128)
            if sub == 0:
                acc[u, rows, :] = out
            else:
                passb[u, rows, :] = out.astype(BF16)
        b_copy(u).start()

    def second_axis(u):
        part, axis, par = part_of(u)
        late = u >= 12
        return jnp.where(axis == 0, jnp.where(late, 0, 1), jnp.where(axis == 1, jnp.where(late, 1, 0), par))

    def to_second(u, v, sign):
        part, axis, par = part_of(u)
        a1, a2, a3 = coords(axis)
        swap = second_axis(u)
        old = jnp.where(swap == 0, a2, a3)
        new = (old + sign * v * (1 - 2 * (old % 2)) + 16) % 4
        return at(axis, a1, jnp.where(swap == 0, new, a2), jnp.where(swap == 0, a3, new), core)

    def to_third(u, v):
        part, axis, par = part_of(u)
        a1, a2, a3 = coords(axis)
        swap = second_axis(u)
        old = jnp.where(swap == 0, a3, a2)
        new = (old + v * (1 - 2 * (old % 2)) + 16) % 4
        return at(axis, a1, jnp.where(swap == 0, a2, new), jnp.where(swap == 0, new, a3), core)

    def turn(u):
        return (u + u // PARTS) % 2

    def c_copy(u):
        return remote(s2.at[u], r2.at[u], c_send, c_recv.at[u], to_second(u, 1, 1 - 2 * turn(u)))

    def phase_c(u):
        swap = second_axis(u)
        par = turn(u)
        all_in(passr.at[u], b_recv.at[u])

        def total(second, third):
            start = second * jnp.where(swap == 0, 128, 32) + third * jnp.where(swap == 0, 32, 128)
            rows = pl.ds(pl.multiple_of(start, 32), 32)
            return acc[u, rows, :] + passr[u, rows, :].astype(F32)

        for third in range(4):
            rows = slice(32 * third, 32 * third + 32)
            s2[u, 0, rows] = total(2 * par, third).astype(BF16)
            s2[u, 1, rows] = total(1, third).astype(BF16)
        c_copy(u).start()
        for third in range(4):
            rows = slice(32 * third, 32 * third + 32)
            acc2[u, 0, rows] = total(3, third)
            acc2[u, 1, rows] = total(2 - 2 * par, third)

    def h_copy(u):
        return remote(t2.at[u], q2.at[u], h_send, h_recv.at[u], to_second(u, 1, 2 * turn(u) - 1))

    def phase_h(u):
        all_in(r2.at[u], c_recv.at[u])
        t2[u] = (acc2[u, 1] + r2[u, 1].astype(F32)).astype(BF16)
        h_copy(u).start()
        acc2[u, 0] = acc2[u, 0] + r2[u, 0].astype(F32)

    def d_copies(u):
        return [
            remote(s3.at[u, d], r3.at[u, d], d_send, d_recv.at[u], to_third(u, d + 1))
            for d in range(3)
        ]

    def phase_d(u):
        all_in(q2.at[u], h_recv.at[u])
        total = acc2[u, 0] + q2[u].astype(F32)
        for d in range(3):
            s3[u, d] = total[32 * d : 32 * d + 32].astype(BF16)
        for copy in d_copies(u):
            copy.start()
        acc3[u] = total[96:128]

    me = blk * 2 + grp

    def e_copy(u, k):
        slot = (me - (u * 8 + k) + 255) % 128
        return remote(sp.at[u, k], rsp.at[slot], e_send, e_recv, (u * 4 + k // 2, k % 2))

    pair_rows = [(0, 0), (1, 0), (2, 0), (1, 6), (0, 2), (1, 2), (2, 2), (0, 4), (1, 4), (0, 6)]

    def phase_e(u):
        all_in(r3.at[u], d_recv.at[u])
        total = acc3[u]
        for d in range(3):
            total = total + r3[u, d].astype(F32)
        ell = (u * LANES + iota((32, 128), 1)).astype(F32)
        total = jnp.where(ell >= morder[...], total, 0.0)
        lanes = pl.ds(pl.multiple_of(u * LANES, LANES), LANES)
        harm_ref[:, lanes] = total
        heavy = total * mweight[...]
        near = [jnp.zeros((8, 128), F32) for _ in range(3)]
        for j in range(4):
            one = total[8 * j : 8 * j + 8]
            weighted = heavy[8 * j : 8 * j + 8]
            for k in range(3):
                other = one if k == 0 else pltpu.roll(one, 8 - 2 * k, 0)
                near[k] = near[k] + weighted * other
        near = [n + pltpu.roll(n, 7, 0) for n in near]
        lane = iota((8, 128), 1) >> 4
        packed = [jnp.zeros((8, 128), F32) for _ in range(2)]
        for p, (k, row) in enumerate(pair_rows):
            moved = near[k] if p % 8 == 0 else pltpu.roll(near[k], 16 * (p % 8), 1)
            wide = jnp.broadcast_to(moved[row : row + 1], (8, 128))
            wide = pltpu.roll(wide, 16, 1, stride=16, stride_axis=0)
            packed[p // 8] = jnp.where(lane == p % 8, wide, packed[p // 8])
        for k in range(8):
            for half in range(2):
                sp[u, k, half : half + 1, :] = packed[half][7 - k : 8 - k]

        for k in range(8):

            @pl.when(u * 8 + k != me)
            def _():
                e_copy(u, k).start()

    def finish():
        arrived = remote(rsp, rsp, e_send, e_recv, device(x, y, z, 1 - core))
        arrived.wait_recv()
        sums = [sp[me // 8, me % 8], rsp[124], rsp[125], rsp[126]]
        for k in range(124):
            sums[k % 4] = sums[k % 4] + rsp[k]
        total = (sums[0] + sums[1]) + (sums[2] + sums[3])
        rows = []
        for half in range(2):
            wide = jnp.broadcast_to(total[half : half + 1], (8, 128))
            wide = pltpu.roll(wide, 16, 1, stride=16, stride_axis=0)
            rows += [wide[7 - p : 8 - p, 0:16] for p in range(8)]
        ell = me * 16 + iota((10, 16), 1)
        power = jnp.concatenate(rows[0:10], axis=0)
        spec_ref[...] = power / (2 * ell + 1).astype(F32)
        arrived.wait_send()

    def orders():
        mine = perm[0, 432:448, :].astype(F32)
        m = jnp.sum(mine * iota((16, 512), 1).astype(F32), axis=1, keepdims=True)
        m = jnp.broadcast_to(m, (16, 128))
        full = jnp.concatenate(
            [jnp.broadcast_to(m[j : j + 1], (8, 128)) for j in range(12, 16)], axis=0
        )
        morder[...] = full
        mweight[...] = jnp.where(full == 0.0, 1.0, 2.0)

    def phase(name, lo, hi, f):
        with jax.named_scope(name):
            loop(lo, hi, f)

    with jax.named_scope("a0"):
        perm_rows(0)
        a_rows(0)
        with jax.named_scope("meet"):
            pl.semaphore_wait(barrier, len(near_by))
        a_start(0)
        perm_rows(1)
        phase_a(2)
        phase_a(1)
        phase_a(3)
        perm_rows(2)
        loop(4, 6, phase_a)
    with jax.named_scope("fourier"):
        fourier()
        f_start()
    phase("a1", 6, 12, phase_a)
    with jax.named_scope("build"):
        for part in range(PARTS):
            build(part)
    phase("bX0", 0, 6, phase_b)
    phase("aX2", 12, 16, phase_a)
    phase("bZ1", 10, 12, phase_b)
    phase("bX1", 6, 10, phase_b)
    with jax.named_scope("orders"):
        orders()
    phase("cX0", 0, 4, phase_c)
    phase("bX2", 12, 16, phase_b)
    phase("cZ0", 4, 6, phase_c)
    phase("cZ1", 10, 12, phase_c)
    phase("hX0", 0, 4, phase_h)
    phase("cX1", 6, 10, phase_c)
    phase("cX2", 12, 16, phase_c)
    phase("hX1", 6, 10, phase_h)
    phase("hZ0", 4, 6, phase_h)
    phase("hZ1", 10, 12, phase_h)
    phase("dX0", 0, 4, phase_d)
    phase("hX2", 12, 16, phase_h)
    phase("dX1", 6, 10, phase_d)
    phase("dZ0", 4, 6, phase_d)
    phase("dZ1", 10, 12, phase_d)
    phase("eX0", 0, 4, phase_e)
    phase("dX2", 12, 16, phase_d)
    phase("e1", 4, 12, phase_e)
    phase("e2", 12, 16, phase_e)
    with jax.named_scope("finish"):
        finish()

    with jax.named_scope("left"):
        all_out(frecv, f_send)
        all_out(recvb, a_send)
        all_out(passb, b_send)
        all_out(s2, c_send)
        all_out(t2, h_send)
        all_out(s3, d_send)


def per_device(sky_maps, legendre, owner_table, table, twiddle):
    vmem = pl.BlockSpec(memory_space=pltpu.VMEM)
    away = pl.BlockSpec(memory_space=pltpu.HBM)
    dma = pltpu.SemaphoreType.DMA
    V = pltpu.VMEM
    inputs = (sky_maps, legendre, owner_table.reshape(1, 512), table, twiddle)
    harm, spectra = pl.pallas_call(
        kernel,
        out_shape=(
            jax.ShapeDtypeStruct((32, 2048), F32),
            jax.ShapeDtypeStruct((10, 16), F32),
        ),
        in_specs=[away] * 5,
        out_specs=(vmem, vmem),
        scratch_shapes=[
            V((4, 4, 4096), F32),
            V((1, 512), jnp.int32),
            V((512, 1024), BF16),
            V((32, 2, 512), F32),
            V((UNITS, 4, 512, 128), BF16),
            V((UNITS, 2, 4, 4, 64, 128), BF16),
            V((UNITS, 3, 2, 4, 64, 128), BF16),
            V((3, 512, 512), BF16),
            V((512, 512), BF16),
            V((PARTS, 8, 128, 256), BF16),
            V((512, 128), F32),
            V((512, 1024), F32),
            V((2, 16, 512), F32),
            V((32, 512), BF16),
            V((PARTS, 32, 128), BF16),
            V((PARTS, 3, 32, 128), BF16),
            V((PARTS, 3, 32, 128), BF16),
            V((UNITS, 512, 128), F32),
            V((UNITS, 512, 128), BF16),
            V((UNITS, 512, 128), BF16),
            V((UNITS, 2, 128, 128), F32),
            V((UNITS, 2, 128, 128), BF16),
            V((UNITS, 2, 128, 128), BF16),
            V((UNITS, 128, 128), BF16),
            V((UNITS, 128, 128), BF16),
            V((UNITS, 32, 128), F32),
            V((UNITS, 3, 32, 128), BF16),
            V((UNITS, 3, 32, 128), BF16),
            V((UNITS, 8, 2, 128), F32),
            V((127, 2, 128), F32),
            V((32, 128), F32),
            V((32, 128), F32),
            dma((4,)), dma((UNITS,)),
            dma, dma((UNITS,)), dma, dma((PARTS,)),
            dma, dma((UNITS,)), dma, dma((UNITS,)), dma, dma((UNITS,)), dma, dma((UNITS,)),
            dma, dma,
        ],
        compiler_params=pltpu.CompilerParams(
            collective_id=0, has_side_effects=True, vmem_limit_bytes=50 * 1024 * 1024
        ),
        name="analysis",
    )(*[pltpu.with_memory_space_constraint(v, pltpu.HBM) for v in inputs])
    return harm.reshape(4, 4, 2, 2048), spectra


def solution(mesh):
    both = ("blk", "grp")
    inner = jax.shard_map(
        per_device,
        mesh=mesh,
        in_specs=(P(None, both, None), P(both, None, None), P(), P(), P()),
        out_specs=(P(both, None, None, None), P(None, both)),
        check_vma=False,
    )

    def run(sky_maps, legendre, owner_table):
        table, twiddle = dft_tables()
        return inner(sky_maps, legendre, owner_table, jnp.asarray(table), jnp.asarray(twiddle))

    return run
```

```python
import functools
import math

import jax
import jax.numpy as jnp
import numpy as np
from jax import lax
from jax.experimental import pallas as pl
from jax.experimental.pallas import tpu as pltpu
from jax.sharding import PartitionSpec as P

MESH = pl.DeviceIdType.MESH
F32 = jnp.float32
BF16 = jnp.bfloat16
UNITS = 16
PARTS = 6
LANES = 128
LATE = 6


def iota(shape, dim):
    return lax.broadcasted_iota(jnp.int32, shape, dim)


def dft_tables():
    k2 = np.arange(128)[:, None]
    m = np.arange(512)[None, :]
    angle = 2.0 * math.pi * ((k2 * m) % 4096) / 4096.0
    table = np.concatenate([np.cos(angle), -np.sin(angle)], axis=1) / 64.0
    k1 = np.arange(32)[:, None]
    turn = 2.0 * math.pi * ((k1 * m) % 32) / 32.0
    twiddle = np.stack([np.cos(turn), np.sin(turn)], axis=1)
    table = table.astype(np.float32)
    high = table.astype(jnp.bfloat16)
    low = (table - high.astype(np.float32)).astype(jnp.bfloat16)
    lane = np.arange(1024)[None, :]
    spread = (lane >> 7) * 16 + (lane & 15) == np.arange(128)[:, None]
    diagonal = (np.arange(128)[:, None] >> 3) == (np.arange(128)[None, :] & 15)
    small = np.concatenate([spread, np.tile(diagonal, (1, 8))], axis=0).astype(jnp.bfloat16)
    return np.concatenate([high, low, small], axis=0), twiddle.astype(np.float32)


def kernel(
    sky_in, leg_ref, own_in, table_in, twid_in, harm_ref, spec_ref,
    sky_ref, own_ref, table_ref, twid_ref, legv, sendb, recvb, perm, amat, fx, fz, fre, fown, fkeep, fsend, frecv,
    acc, passb, passr, acc2, s2, r2, t2, q2, acc3, s3, r3, sp, rsp, morder, mweight,
    in_sem, leg_sem, a_send, a_recv, f_send, f_recv, b_send, b_recv, c_send, c_recv,
    h_send, h_recv, d_send, d_recv, e_send, e_recv,
):
    blk = lax.axis_index("blk")
    grp = lax.axis_index("grp")
    x = blk // 16
    y = (blk // 4) % 4
    z = grp * 2 + (blk // 2) % 2
    core = blk % 2

    def pick(axis, v0, v1, v2):
        return jnp.where(axis == 0, v0, jnp.where(axis == 1, v1, v2))

    def coords(axis):
        return pick(axis, x, y, z), pick(axis, y, z, x), pick(axis, z, x, y)

    def device(xx, yy, zz, cc):
        return (xx * 16 + yy * 4 + (zz % 2) * 2 + cc, zz // 2)

    def at(axis, v1, v2, v3, cc):
        return device(pick(axis, v1, v3, v2), pick(axis, v2, v1, v3), pick(axis, v3, v2, v1), cc)

    def part_of(u, c=core):
        late = jnp.where(u == 12, 0, jnp.where(u == 13, 1 + 2 * c, jnp.where(u == 14, 2, 4 + c)))
        part = jnp.where(u < 12, u % PARTS, late)
        return part, part // 2, part % 2

    def pairs(axis, par):
        a1, a2, a3 = coords(axis)
        step = (1 - 2 * (a1 % 2)) * (1 - 2 * par)
        first = (a1 + step + 4) % 4
        second = (a1 - step + 4) % 4
        return a1, a2, a3, first, second

    def remote(src, dst, ss, rs, dev):
        return pltpu.make_async_remote_copy(
            src_ref=src, dst_ref=dst, send_sem=ss, recv_sem=rs, device_id=dev, device_id_type=MESH
        )

    def loop(lo, hi, f):
        def body(i, c):
            f(i)
            return c

        lax.fori_loop(lo, hi, body, 0)

    barrier = pltpu.get_barrier_semaphore()
    near_by = [device(x, y, z, 1 - core)]
    for axis in range(3):
        a1, a2, a3 = coords(axis)
        for d in (1, 2, 3):
            near_by.append(at(axis, (a1 + d) % 4, a2, a3, core))
            if d != 2:
                near_by.append(at(axis, (a1 + d) % 4, a2, a3, 1 - core))
    for dev in near_by:
        pl.semaphore_signal(barrier, inc=1, device_id=dev, device_id_type=MESH)

    def leg_copy(u):
        lanes = pl.ds(pl.multiple_of(u * LANES, LANES), LANES)
        return pltpu.make_async_copy(leg_ref.at[:, :, lanes], legv.at[u], leg_sem.at[u])

    inputs = [
        pltpu.make_async_copy(src, dst, in_sem.at[i])
        for i, (src, dst) in enumerate(
            [(own_in, own_ref), (sky_in, sky_ref), (table_in, table_ref), (twid_in, twid_ref)]
        )
    ]
    inputs[0].start()
    loop(0, PARTS, lambda u: leg_copy(u).start())
    for copy in inputs[1:]:
        copy.start()
    loop(PARTS, UNITS, lambda u: leg_copy(u).start())

    def perm_rows(axis):
        a1, a2, a3 = coords(axis)
        i = iota((512, 128), 0)
        v3 = (a3 + ((i >> 2) + 1) * (1 - 2 * (a3 % 2)) + 512) & 3
        v2 = (a2 + ((i >> 4) + 1) * (1 - 2 * (a2 % 2)) + 128) & 3
        v1 = (a1 + (((i >> 6) & 3) + 1) * (1 - 2 * (a1 % 2)) + 16) & 3
        cc = core ^ (i >> 8)
        xx, yy, zz = ((v1, v2, v3), (v3, v1, v2), (v2, v3, v1))[axis]
        slot = (xx << 7) + (yy << 5) + ((zz & 1) << 4) + (cc << 3) + ((zz >> 1) << 2) + (i & 3)
        slot = slot - iota((512, 128), 1)
        chosen = jnp.concatenate(
            [jnp.where(slot == k * 128, 1.0, 0.0).astype(BF16) for k in range(4)], axis=1
        )
        if axis == 0:
            inputs[0].wait()
        order = own_ref[...]
        row = iota((8, 512), 0)
        digits = jnp.where(row == 0, order & 255, jnp.where(row == 1, order >> 8, 0))
        codes = lax.dot_general(
            chosen, digits.astype(F32).astype(BF16), (((1,), (1,)), ((), ())),
            preferred_element_type=F32,
        )
        orders_of = codes[:, 0:1] + 256.0 * codes[:, 1:2]
        for k in range(4):
            m = (iota((512, 128), 1) + k * 128).astype(F32)
            perm[axis, :, k * 128 : k * 128 + 128] = jnp.where(m == orders_of, 1.0, 0.0).astype(BF16)

    def a_copies(u):
        part, axis, par = part_of(u)
        a1, a2, a3, first, _ = pairs(axis, par)
        _, axis_o, par_o = part_of(u, 1 - core)
        _, b2, b3, first_o, _ = pairs(axis_o, par_o)
        sem = a_recv.at[u]
        return (
            remote(sendb.at[u, 0, pl.ds(0, 2)], recvb.at[u, 1], a_send, sem,
                   at(axis, first, a2, a3, core)),
            remote(sendb.at[u, 1, pl.ds(0, 2)], recvb.at[u, 2], a_send, sem,
                   at(axis_o, first_o, b2, b3, 1 - core)),
            remote(sendb.at[u, 1, pl.ds(2, 2)], recvb.at[u, 0], a_send, sem,
                   device(x, y, z, 1 - core)),
        )

    def a_rows(u):
        leg_copy(u).wait()
        kinds = [part_of(u, core), part_of(u, 1 - core)]
        for pair in range(2):
            wide = jnp.concatenate([legv[u, 2 * pair], legv[u, 2 * pair + 1]], axis=1)
            for rc, (_, axis, par) in enumerate(kinds):
                roles = (3 * par, 1, 3 - 3 * par, 2)
                chosen = perm[axis, rc * 256 : rc * 256 + 256, :]
                rows = jnp.dot(chosen, wide, preferred_element_type=F32).astype(BF16)
                for rel in range(4):
                    piece = rows[rel * 64 : rel * 64 + 64]
                    sendb[u, rc, roles[rel], 2 * pair] = piece[:, :128]
                    sendb[u, rc, roles[rel], 2 * pair + 1] = piece[:, 128:]

    def a_start(u):
        for copy in a_copies(u):
            copy.start()

    def phase_a(u):
        a_rows(u)
        a_start(u)

    def all_in(ref, sem):
        remote(ref, ref, a_send, sem, device(x, y, z, 1 - core)).wait_recv()

    def all_out(ref, sem):
        remote(ref, ref, sem, e_recv, device(x, y, z, 1 - core)).wait_send()

    def fourier():
        for copy in inputs[1:]:
            copy.wait()
        for a in range(4):
            for k1 in range(32):
                fx[k1 * 16 + a * 4 : k1 * 16 + a * 4 + 4, :] = sky_ref[
                    a, :, k1 * 128 : (k1 + 1) * 128
                ]

        def rows_of(i):
            rows = pl.ds(pl.multiple_of(i * 128, 128), 128)
            pixels = fx[rows, :]
            high = pixels.astype(BF16)
            low = (pixels - high.astype(F32)).astype(BF16)
            table = table_ref[0:128, :]
            fz[rows, :] = jnp.dot(
                jnp.concatenate([high, low], axis=1), jnp.concatenate([table, table], axis=0),
                preferred_element_type=F32,
            ) + jnp.dot(high, table_ref[128:256, :], preferred_element_type=F32)

        loop(0, 4, rows_of)

        def add(k1, sums):
            re, im = sums
            rows = pl.ds(pl.multiple_of(k1 * 16, 16), 16)
            zr = fz[rows, 0:512]
            zi = fz[rows, 512:1024]
            c = twid_ref[k1, 0:1, :]
            s = twid_ref[k1, 1:2, :]
            return re + (zr * c + zi * s), im + (zi * c - zr * s)

        zero = jnp.zeros((16, 512), F32)
        re, im = lax.fori_loop(0, 32, add, (zero, zero))
        fre[0] = re
        fre[1] = im
        for r in range(4):
            rows = [fre[q, a * 4 + r : a * 4 + r + 1, :] for a in range(4) for q in range(2)]
            fown[r * 8 : r * 8 + 8, :] = jnp.concatenate(rows, axis=0).astype(BF16)

    def f_copies(part):
        axis, par = part // 2, part % 2
        a1, a2, a3, first, _ = pairs(axis, par)
        sem = f_recv.at[part]
        return (
            remote(fsend.at[part, 0], frecv.at[part, 1], f_send, sem, at(axis, first, a2, a3, core)),
            remote(fsend.at[part, 1], frecv.at[part, 2], f_send, sem,
                   at(axis, first, a2, a3, 1 - core)),
            remote(fsend.at[part, 2], frecv.at[part, 0], f_send, sem,
                   at(axis, a1, a2, a3, 1 - core)),
        )

    def f_start():
        low = iota((32, 128), 1) < 64
        for axis in range(3):
            cols = lax.dot_general(
                fown[...], perm[axis], (((1,), (1,)), ((), ())), preferred_element_type=F32
            )
            tile = [cols[:, k * 128 : k * 128 + 128] for k in range(4)]
            turned = [pltpu.roll(t, 64, 1) for t in tile]

            def half(rel, rc, side):
                return (tile if rel % 2 == side else turned)[2 * rc + rel // 2]

            def joined(mine, passed, rc):
                return jnp.where(low, half(mine, rc, 0), half(passed, rc, 1)).astype(BF16)

            for par in range(2):
                part = 2 * axis + par
                fsend[part, 0] = joined(2 * par, 1, 0)
                fsend[part, 1] = joined(2 * par, 1, 1)
                fsend[part, 2] = joined(3, 2 - 2 * par, 1)
                fkeep[part] = joined(3, 2 - 2 * par, 0)
                for copy in f_copies(part):
                    copy.start()

    def build(part):
        all_in(frecv.at[part], f_recv.at[part])
        picked = jnp.concatenate([fkeep[part]] + [frecv[part, k] for k in range(3)], axis=0)
        tiled = jnp.dot(picked, table_ref[256:384, :], preferred_element_type=F32)
        group = iota((8, 128), 1) >> 4
        for g in range(8):
            for h in range(2):
                base = tiled[64 * h : 64 * h + 8, g * 128 : g * 128 + 128]
                for i in range(1, 8):
                    row = (8 * h + i) * 8
                    base = jnp.where(
                        group == i, tiled[row : row + 8, g * 128 : g * 128 + 128], base
                    )
                two = jnp.concatenate([base, base], axis=0).astype(BF16)
                for k in range(8):
                    rows = slice(16 * k, 16 * k + 16)
                    amat[part, g, rows, h * 128 : h * 128 + 128] = (
                        two * table_ref[384 + 16 * k : 400 + 16 * k, 0:128]
                    )

    def b_copy(u):
        part, axis, par = part_of(u)
        _, a2, a3, _, second = pairs(axis, par)
        return remote(passb.at[u], passr.at[u], b_send, b_recv.at[u],
                      at(axis, second, a2, a3, core))

    def phase_b(u):
        part, axis, par = part_of(u)
        all_in(recvb.at[u], a_recv.at[u])
        for g in range(8):
            sub, low = g // 4, 16 * (g % 4)
            slabs = [sendb[u, 0, 2 + sub, r, low : low + 16, :] for r in range(4)]
            for src in range(3):
                slabs += [recvb[u, src, sub, r, low : low + 16, :] for r in range(4)]
            out = jnp.dot(
                amat[part, g], jnp.concatenate(slabs, axis=0), preferred_element_type=F32
            )
            rows = slice((g % 4) * 128, (g % 4) * 128 + 128)
            if sub == 0:
                acc[u, rows, :] = out
            else:
                passb[u, rows, :] = out.astype(BF16)
        b_copy(u).start()

    def second_axis(u):
        part, axis, par = part_of(u)
        late = jnp.where(u >= LATE, 1, 0)
        return jnp.where(axis == 0, 1 - late, jnp.where(axis == 1, late, par))

    def to_second(u, v, sign):
        part, axis, par = part_of(u)
        a1, a2, a3 = coords(axis)
        swap = second_axis(u)
        old = jnp.where(swap == 0, a2, a3)
        new = (old + sign * v * (1 - 2 * (old % 2)) + 16) % 4
        return at(axis, a1, jnp.where(swap == 0, new, a2), jnp.where(swap == 0, a3, new), core)

    def to_third(u, v):
        part, axis, par = part_of(u)
        a1, a2, a3 = coords(axis)
        swap = second_axis(u)
        old = jnp.where(swap == 0, a3, a2)
        new = (old + v * (1 - 2 * (old % 2)) + 16) % 4
        return at(axis, a1, jnp.where(swap == 0, a2, new), jnp.where(swap == 0, new, a3), core)

    def turn(u):
        return (part_of(u)[2] + u // PARTS) % 2

    def c_copy(u):
        return remote(s2.at[u], r2.at[u], c_send, c_recv.at[u], to_second(u, 1, 1 - 2 * turn(u)))

    def phase_c(u):
        swap = second_axis(u)
        par = turn(u)
        all_in(passr.at[u], b_recv.at[u])

        def total(second, third):
            start = second * jnp.where(swap == 0, 128, 32) + third * jnp.where(swap == 0, 32, 128)
            rows = pl.ds(pl.multiple_of(start, 32), 32)
            return acc[u, rows, :] + passr[u, rows, :].astype(F32)

        for third in range(4):
            rows = slice(32 * third, 32 * third + 32)
            s2[u, 0, rows] = total(2 * par, third).astype(BF16)
            s2[u, 1, rows] = total(1, third).astype(BF16)
        c_copy(u).start()
        for third in range(4):
            rows = slice(32 * third, 32 * third + 32)
            acc2[u, 0, rows] = total(3, third)
            acc2[u, 1, rows] = total(2 - 2 * par, third)

    def h_copy(u):
        return remote(t2.at[u], q2.at[u], h_send, h_recv.at[u], to_second(u, 1, 2 * turn(u) - 1))

    def phase_h(u):
        all_in(r2.at[u], c_recv.at[u])
        t2[u] = (acc2[u, 1] + r2[u, 1].astype(F32)).astype(BF16)
        h_copy(u).start()
        acc2[u, 0] = acc2[u, 0] + r2[u, 0].astype(F32)

    def d_copies(u):
        return [
            remote(s3.at[u, d], r3.at[u, d], d_send, d_recv.at[u], to_third(u, d + 1))
            for d in range(3)
        ]

    def phase_d(u):
        all_in(q2.at[u], h_recv.at[u])
        total = acc2[u, 0] + q2[u].astype(F32)
        for d in range(3):
            s3[u, d] = total[32 * d : 32 * d + 32].astype(BF16)
        for copy in d_copies(u):
            copy.start()
        acc3[u] = total[96:128]

    me = blk * 2 + grp

    def e_copy(u, k):
        slot = (me - (u * 8 + k) + 255) % 128
        return remote(sp.at[u, k], rsp.at[slot], e_send, e_recv, (u * 4 + k // 2, k % 2))

    pair_rows = [(0, 0), (1, 0), (2, 0), (1, 6), (0, 2), (1, 2), (2, 2), (0, 4), (1, 4), (0, 6)]

    def e_sums(u):
        total = acc3[u]
        for d in range(3):
            total = total + r3[u, d].astype(F32)
        ell = (u * LANES + iota((32, 128), 1)).astype(F32)
        total = jnp.where(ell >= morder[...], total, 0.0)
        lanes = pl.ds(pl.multiple_of(u * LANES, LANES), LANES)
        harm_ref[:, lanes] = total
        heavy = total * mweight[...]
        near = [jnp.zeros((8, 128), F32) for _ in range(3)]
        for j in range(4):
            one = total[8 * j : 8 * j + 8]
            weighted = heavy[8 * j : 8 * j + 8]
            for k in range(3):
                other = one if k == 0 else pltpu.roll(one, 8 - 2 * k, 0)
                near[k] = near[k] + weighted * other
        near = [n + pltpu.roll(n, 7, 0) for n in near]
        lane = iota((8, 128), 1) >> 4
        packed = [jnp.zeros((8, 128), F32) for _ in range(2)]
        for p, (k, row) in enumerate(pair_rows):
            moved = near[k] if p % 8 == 0 else pltpu.roll(near[k], 16 * (p % 8), 1)
            wide = jnp.broadcast_to(moved[row : row + 1], (8, 128))
            wide = pltpu.roll(wide, 16, 1, stride=16, stride_axis=0)
            packed[p // 8] = jnp.where(lane == p % 8, wide, packed[p // 8])
        for k in range(8):
            for half in range(2):
                sp[u, k, half : half + 1, :] = packed[half][7 - k : 8 - k]

    def e_start(u):
        @pl.when(u != me // 8)
        def _():
            for k in range(8):
                e_copy(u, k).start()

        @pl.when(u == me // 8)
        def _():
            def send(k):
                @pl.when(k != me % 8)
                def _():
                    e_copy(u, k).start()

            loop(0, 8, send)

    def phase_e(lo, hi):
        for u in range(lo, hi):
            all_in(r3.at[u], d_recv.at[u])
        for u in range(lo, hi):
            e_sums(u)
        for u in range(lo, hi):
            e_start(u)

    def finish():
        arrived = remote(rsp, rsp, e_send, e_recv, device(x, y, z, 1 - core))
        arrived.wait_recv()
        sums = [sp[me // 8, me % 8], rsp[124], rsp[125], rsp[126]]
        for k in range(124):
            sums[k % 4] = sums[k % 4] + rsp[k]
        total = (sums[0] + sums[1]) + (sums[2] + sums[3])
        rows = []
        for half in range(2):
            wide = jnp.broadcast_to(total[half : half + 1], (8, 128))
            wide = pltpu.roll(wide, 16, 1, stride=16, stride_axis=0)
            rows += [wide[7 - p : 8 - p, 0:16] for p in range(8)]
        ell = me * 16 + iota((10, 16), 1)
        power = jnp.concatenate(rows[0:10], axis=0)
        spec_ref[...] = power / (2 * ell + 1).astype(F32)
        arrived.wait_send()

    def orders():
        mine = perm[0, 240:256, :].astype(F32)
        m = jnp.sum(mine * iota((16, 512), 1).astype(F32), axis=1, keepdims=True)
        m = jnp.broadcast_to(m, (16, 128))
        full = jnp.concatenate(
            [jnp.broadcast_to(m[j : j + 1], (8, 128)) for j in range(12, 16)], axis=0
        )
        morder[...] = full
        mweight[...] = jnp.where(full == 0.0, 1.0, 2.0)

    def phase(name, lo, hi, f):
        with jax.named_scope(name):
            loop(lo, hi, f)

    with jax.named_scope("a0"):
        perm_rows(0)
        a_rows(0)
        with jax.named_scope("meet"):
            pl.semaphore_wait(barrier, len(near_by))
        a_start(0)
        perm_rows(1)
        phase_a(2)
        phase_a(1)
        phase_a(3)
        perm_rows(2)
        loop(4, 6, phase_a)
    with jax.named_scope("fourier"):
        fourier()
        f_start()
    phase("a1", 6, 7, phase_a)
    phase_a(8)
    phase_a(7)
    phase("a2", 9, 16, phase_a)
    with jax.named_scope("orders"):
        orders()
    with jax.named_scope("build"):
        for part in range(PARTS):
            build(part)
    phase("b0", 0, 6, phase_b)
    phase("b1", 6, 12, phase_b)
    phase("bX2", 12, 16, phase_b)
    phase("cX0", 0, 4, phase_c)
    phase("cZ0", 4, 6, phase_c)
    phase("cX1", 6, 10, phase_c)
    phase("cZ1", 10, 12, phase_c)
    phase("cX2", 12, 16, phase_c)
    phase("hX0", 0, 4, phase_h)
    phase("hZ0", 4, 6, phase_h)
    phase("hZ1", 10, 12, phase_h)
    phase("hX1", 6, 10, phase_h)
    phase("hX2", 12, 16, phase_h)
    phase("dX0", 0, 4, phase_d)
    phase("dZ0", 4, 6, phase_d)
    phase("dZ1", 10, 12, phase_d)
    phase("dX1", 6, 10, phase_d)
    phase("dX2", 12, 16, phase_d)
    for name, lo, hi in (("eX0", 0, 4), ("eZ0", 4, 6), ("eX1", 6, 10), ("eZ1", 10, 12), ("eX2", 12, 16)):
        with jax.named_scope(name):
            phase_e(lo, hi)
    with jax.named_scope("finish"):
        finish()

    with jax.named_scope("left"):
        all_out(frecv, f_send)
        all_out(recvb, a_send)
        all_out(passb, b_send)
        all_out(s2, c_send)
        all_out(t2, h_send)
        all_out(s3, d_send)


def per_device(sky_maps, legendre, owner_table, table, twiddle):
    vmem = pl.BlockSpec(memory_space=pltpu.VMEM)
    away = pl.BlockSpec(memory_space=pltpu.HBM)
    dma = pltpu.SemaphoreType.DMA
    V = pltpu.VMEM
    inputs = (sky_maps, legendre, owner_table.reshape(1, 512), table, twiddle)
    harm, spectra = pl.pallas_call(
        kernel,
        out_shape=(
            jax.ShapeDtypeStruct((32, 2048), F32),
            jax.ShapeDtypeStruct((10, 16), F32),
        ),
        in_specs=[away] * 5,
        out_specs=(vmem, vmem),
        scratch_shapes=[
            V((4, 4, 4096), F32),
            V((1, 512), jnp.int32),
            V((512, 1024), BF16),
            V((32, 2, 512), F32),
            V((UNITS, 4, 512, 128), BF16),
            V((UNITS, 2, 4, 4, 64, 128), BF16),
            V((UNITS, 3, 2, 4, 64, 128), BF16),
            V((3, 512, 512), BF16),
            V((PARTS, 8, 128, 256), BF16),
            V((512, 128), F32),
            V((512, 1024), F32),
            V((2, 16, 512), F32),
            V((32, 512), BF16),
            V((PARTS, 32, 128), BF16),
            V((PARTS, 3, 32, 128), BF16),
            V((PARTS, 3, 32, 128), BF16),
            V((UNITS, 512, 128), F32),
            V((UNITS, 512, 128), BF16),
            V((UNITS, 512, 128), BF16),
            V((UNITS, 2, 128, 128), F32),
            V((UNITS, 2, 128, 128), BF16),
            V((UNITS, 2, 128, 128), BF16),
            V((UNITS, 128, 128), BF16),
            V((UNITS, 128, 128), BF16),
            V((UNITS, 32, 128), F32),
            V((UNITS, 3, 32, 128), BF16),
            V((UNITS, 3, 32, 128), BF16),
            V((UNITS, 8, 2, 128), F32),
            V((127, 2, 128), F32),
            V((32, 128), F32),
            V((32, 128), F32),
            dma((4,)), dma((UNITS,)),
            dma, dma((UNITS,)), dma, dma((PARTS,)),
            dma, dma((UNITS,)), dma, dma((UNITS,)), dma, dma((UNITS,)), dma, dma((UNITS,)),
            dma, dma,
        ],
        compiler_params=pltpu.CompilerParams(
            collective_id=0, has_side_effects=True, vmem_limit_bytes=50 * 1024 * 1024
        ),
        name="analysis",
    )(*[pltpu.with_memory_space_constraint(v, pltpu.HBM) for v in inputs])
    return harm.reshape(4, 4, 2, 2048), spectra


def solution(mesh):
    both = ("blk", "grp")
    inner = jax.shard_map(
        per_device,
        mesh=mesh,
        in_specs=(P(None, both, None), P(both, None, None), P(), P(), P()),
        out_specs=(P(both, None, None, None), P(None, both)),
        check_vma=False,
    )

    def run(sky_maps, legendre, owner_table):
        table, twiddle = dft_tables()
        return inner(sky_maps, legendre, owner_table, jnp.asarray(table), jnp.asarray(twiddle))

    return run
```

```python
import functools
import math

import jax
import jax.numpy as jnp
import numpy as np
from jax import lax
from jax.experimental import pallas as pl
from jax.experimental.pallas import tpu as pltpu
from jax.sharding import PartitionSpec as P

MESH = pl.DeviceIdType.MESH
F32 = jnp.float32
BF16 = jnp.bfloat16
UNITS = 16
PARTS = 6
LANES = 128
LATE = 6


def iota(shape, dim):
    return lax.broadcasted_iota(jnp.int32, shape, dim)


def dft_tables():
    k2 = np.arange(128)[:, None]
    m = np.arange(512)[None, :]
    angle = 2.0 * math.pi * ((k2 * m) % 4096) / 4096.0
    table = np.concatenate([np.cos(angle), -np.sin(angle)], axis=1) / 64.0
    k1 = np.arange(32)[:, None]
    turn = 2.0 * math.pi * ((k1 * m) % 32) / 32.0
    twiddle = np.stack([np.cos(turn), np.sin(turn)], axis=1)
    table = table.astype(np.float32)
    high = table.astype(jnp.bfloat16)
    low = (table - high.astype(np.float32)).astype(jnp.bfloat16)
    lane = np.arange(1024)[None, :]
    spread = (lane >> 7) * 16 + (lane & 15) == np.arange(128)[:, None]
    diagonal = (np.arange(128)[:, None] >> 3) == (np.arange(128)[None, :] & 15)
    small = np.concatenate([spread, np.tile(diagonal, (1, 8))], axis=0).astype(jnp.bfloat16)
    return np.concatenate([high, low, small], axis=0), twiddle.astype(np.float32)


def kernel(
    sky_in, leg_ref, own_in, table_in, twid_in, harm_ref, spec_ref,
    sky_ref, own_ref, table_ref, twid_ref, legv, sendb, recvb, perm, amat, fx, fz, fre, fown, fkeep, fsend, frecv,
    acc, passb, passr, acc2, s2, r2, t2, q2, acc3, s3, r3, sp, rsp, morder, mweight,
    in_sem, leg_sem, a_send, a_recv, f_send, f_recv, b_send, b_recv, c_send, c_recv,
    h_send, h_recv, d_send, d_recv, e_send, e_recv,
):
    blk = lax.axis_index("blk")
    grp = lax.axis_index("grp")
    x = blk // 16
    y = (blk // 4) % 4
    z = grp * 2 + (blk // 2) % 2
    core = blk % 2

    def pick(axis, v0, v1, v2):
        return jnp.where(axis == 0, v0, jnp.where(axis == 1, v1, v2))

    def coords(axis):
        return pick(axis, x, y, z), pick(axis, y, z, x), pick(axis, z, x, y)

    def device(xx, yy, zz, cc):
        return (xx * 16 + yy * 4 + (zz % 2) * 2 + cc, zz // 2)

    def at(axis, v1, v2, v3, cc):
        return device(pick(axis, v1, v3, v2), pick(axis, v2, v1, v3), pick(axis, v3, v2, v1), cc)

    def part_of(u, c=core):
        late = jnp.where(u == 12, 0, jnp.where(u == 13, 1 + 2 * c, jnp.where(u == 14, 2, 4 + c)))
        part = jnp.where(u < 12, u % PARTS, late)
        return part, part // 2, part % 2

    def pairs(axis, par):
        a1, a2, a3 = coords(axis)
        step = (1 - 2 * (a1 % 2)) * (1 - 2 * par)
        first = (a1 + step + 4) % 4
        second = (a1 - step + 4) % 4
        return a1, a2, a3, first, second

    def remote(src, dst, ss, rs, dev):
        return pltpu.make_async_remote_copy(
            src_ref=src, dst_ref=dst, send_sem=ss, recv_sem=rs, device_id=dev, device_id_type=MESH
        )

    def loop(lo, hi, f):
        def body(i, c):
            f(i)
            return c

        lax.fori_loop(lo, hi, body, 0)

    barrier = pltpu.get_barrier_semaphore()
    near_by = [device(x, y, z, 1 - core)]
    for axis in range(3):
        a1, a2, a3 = coords(axis)
        for d in (1, 2, 3):
            near_by.append(at(axis, (a1 + d) % 4, a2, a3, core))
            if d != 2:
                near_by.append(at(axis, (a1 + d) % 4, a2, a3, 1 - core))
    for dev in near_by:
        pl.semaphore_signal(barrier, inc=1, device_id=dev, device_id_type=MESH)

    def leg_copy(u):
        lanes = pl.ds(pl.multiple_of(u * LANES, LANES), LANES)
        return pltpu.make_async_copy(leg_ref.at[:, :, lanes], legv.at[u], leg_sem.at[u])

    inputs = [
        pltpu.make_async_copy(src, dst, in_sem.at[i])
        for i, (src, dst) in enumerate(
            [(own_in, own_ref), (sky_in, sky_ref), (table_in, table_ref), (twid_in, twid_ref)]
        )
    ]
    inputs[0].start()
    loop(0, PARTS, lambda u: leg_copy(u).start())
    for copy in inputs[1:]:
        copy.start()
    loop(PARTS, UNITS, lambda u: leg_copy(u).start())

    def perm_rows(axis):
        a1, a2, a3 = coords(axis)
        i = iota((512, 128), 0)
        v3 = (a3 + ((i >> 2) + 1) * (1 - 2 * (a3 % 2)) + 512) & 3
        v2 = (a2 + ((i >> 4) + 1) * (1 - 2 * (a2 % 2)) + 128) & 3
        v1 = (a1 + (((i >> 6) & 3) + 1) * (1 - 2 * (a1 % 2)) + 16) & 3
        cc = core ^ (i >> 8)
        xx, yy, zz = ((v1, v2, v3), (v3, v1, v2), (v2, v3, v1))[axis]
        slot = (xx << 7) + (yy << 5) + ((zz & 1) << 4) + (cc << 3) + ((zz >> 1) << 2) + (i & 3)
        slot = slot - iota((512, 128), 1)
        chosen = jnp.concatenate(
            [jnp.where(slot == k * 128, 1.0, 0.0).astype(BF16) for k in range(4)], axis=1
        )
        if axis == 0:
            inputs[0].wait()
        order = own_ref[...]
        row = iota((8, 512), 0)
        digits = jnp.where(row == 0, order & 255, jnp.where(row == 1, order >> 8, 0))
        codes = lax.dot_general(
            chosen, digits.astype(F32).astype(BF16), (((1,), (1,)), ((), ())),
            preferred_element_type=F32,
        )
        orders_of = codes[:, 0:1] + 256.0 * codes[:, 1:2]
        for k in range(4):
            m = (iota((512, 128), 1) + k * 128).astype(F32)
            perm[axis, :, k * 128 : k * 128 + 128] = jnp.where(m == orders_of, 1.0, 0.0).astype(BF16)

    def a_copies(u):
        part, axis, par = part_of(u)
        a1, a2, a3, first, _ = pairs(axis, par)
        _, axis_o, par_o = part_of(u, 1 - core)
        _, b2, b3, first_o, _ = pairs(axis_o, par_o)
        sem = a_recv.at[u]
        return (
            remote(sendb.at[u, 0, pl.ds(0, 2)], recvb.at[u, 1], a_send, sem,
                   at(axis, first, a2, a3, core)),
            remote(sendb.at[u, 1, pl.ds(0, 2)], recvb.at[u, 2], a_send, sem,
                   at(axis_o, first_o, b2, b3, 1 - core)),
            remote(sendb.at[u, 1, pl.ds(2, 2)], recvb.at[u, 0], a_send, sem,
                   device(x, y, z, 1 - core)),
        )

    def a_rows(u):
        leg_copy(u).wait()
        kinds = [part_of(u, core), part_of(u, 1 - core)]
        for pair in range(2):
            wide = jnp.concatenate([legv[u, 2 * pair], legv[u, 2 * pair + 1]], axis=1)
            for rc, (_, axis, par) in enumerate(kinds):
                roles = (3 * par, 1, 3 - 3 * par, 2)
                chosen = perm[axis, rc * 256 : rc * 256 + 256, :]
                rows = jnp.dot(chosen, wide, preferred_element_type=F32).astype(BF16)
                for rel in range(4):
                    piece = rows[rel * 64 : rel * 64 + 64]
                    sendb[u, rc, roles[rel], 2 * pair] = piece[:, :128]
                    sendb[u, rc, roles[rel], 2 * pair + 1] = piece[:, 128:]

    def a_start(u):
        for copy in a_copies(u):
            copy.start()

    def phase_a(u):
        a_rows(u)
        a_start(u)

    def all_in(ref, sem):
        remote(ref, ref, a_send, sem, device(x, y, z, 1 - core)).wait_recv()

    def all_out(ref, sem):
        remote(ref, ref, sem, e_recv, device(x, y, z, 1 - core)).wait_send()

    def fourier():
        for copy in inputs[1:]:
            copy.wait()
        for a in range(4):
            for k1 in range(32):
                fx[k1 * 16 + a * 4 : k1 * 16 + a * 4 + 4, :] = sky_ref[
                    a, :, k1 * 128 : (k1 + 1) * 128
                ]

        def rows_of(i):
            rows = pl.ds(pl.multiple_of(i * 128, 128), 128)
            pixels = fx[rows, :]
            high = pixels.astype(BF16)
            low = (pixels - high.astype(F32)).astype(BF16)
            table = table_ref[0:128, :]
            fz[rows, :] = jnp.dot(
                jnp.concatenate([high, low], axis=1), jnp.concatenate([table, table], axis=0),
                preferred_element_type=F32,
            ) + jnp.dot(high, table_ref[128:256, :], preferred_element_type=F32)

        for i in range(4):
            rows_of(i)

        def add(k1, sums):
            re, im = sums
            rows = pl.ds(pl.multiple_of(k1 * 16, 16), 16)
            zr = fz[rows, 0:512]
            zi = fz[rows, 512:1024]
            c = twid_ref[k1, 0:1, :]
            s = twid_ref[k1, 1:2, :]
            return re + (zr * c + zi * s), im + (zi * c - zr * s)

        zero = jnp.zeros((16, 512), F32)
        re, im = lax.fori_loop(0, 32, add, (zero, zero), unroll=8)
        fre[0] = re
        fre[1] = im
        for r in range(4):
            rows = [fre[q, a * 4 + r : a * 4 + r + 1, :] for a in range(4) for q in range(2)]
            fown[r * 8 : r * 8 + 8, :] = jnp.concatenate(rows, axis=0).astype(BF16)

    def f_copies(part):
        axis, par = part // 2, part % 2
        a1, a2, a3, first, _ = pairs(axis, par)
        sem = f_recv.at[part]
        return (
            remote(fsend.at[part, 0], frecv.at[part, 1], f_send, sem, at(axis, first, a2, a3, core)),
            remote(fsend.at[part, 1], frecv.at[part, 2], f_send, sem,
                   at(axis, first, a2, a3, 1 - core)),
            remote(fsend.at[part, 2], frecv.at[part, 0], f_send, sem,
                   at(axis, a1, a2, a3, 1 - core)),
        )

    def f_start():
        low = iota((32, 128), 1) < 64
        for axis in range(3):
            cols = lax.dot_general(
                fown[...], perm[axis], (((1,), (1,)), ((), ())), preferred_element_type=F32
            )
            tile = [cols[:, k * 128 : k * 128 + 128] for k in range(4)]
            turned = [pltpu.roll(t, 64, 1) for t in tile]

            def half(rel, rc, side):
                return (tile if rel % 2 == side else turned)[2 * rc + rel // 2]

            def joined(mine, passed, rc):
                return jnp.where(low, half(mine, rc, 0), half(passed, rc, 1)).astype(BF16)

            for par in range(2):
                part = 2 * axis + par
                fsend[part, 0] = joined(2 * par, 1, 0)
                fsend[part, 1] = joined(2 * par, 1, 1)
                fsend[part, 2] = joined(3, 2 - 2 * par, 1)
                fkeep[part] = joined(3, 2 - 2 * par, 0)
                for copy in f_copies(part):
                    copy.start()

    def build(part):
        all_in(frecv.at[part], f_recv.at[part])
        picked = jnp.concatenate([fkeep[part]] + [frecv[part, k] for k in range(3)], axis=0)
        tiled = jnp.dot(picked, table_ref[256:384, :], preferred_element_type=F32)
        group = iota((8, 128), 1) >> 4
        for g in range(8):
            for h in range(2):
                base = tiled[64 * h : 64 * h + 8, g * 128 : g * 128 + 128]
                for i in range(1, 8):
                    row = (8 * h + i) * 8
                    base = jnp.where(
                        group == i, tiled[row : row + 8, g * 128 : g * 128 + 128], base
                    )
                two = jnp.concatenate([base, base], axis=0).astype(BF16)
                for k in range(8):
                    rows = slice(16 * k, 16 * k + 16)
                    amat[part, g, rows, h * 128 : h * 128 + 128] = (
                        two * table_ref[384 + 16 * k : 400 + 16 * k, 0:128]
                    )

    def b_copy(u):
        part, axis, par = part_of(u)
        _, a2, a3, _, second = pairs(axis, par)
        return remote(passb.at[u], passr.at[u], b_send, b_recv.at[u],
                      at(axis, second, a2, a3, core))

    def phase_b(u):
        part, axis, par = part_of(u)
        all_in(recvb.at[u], a_recv.at[u])
        for g in range(8):
            sub, low = g // 4, 16 * (g % 4)
            slabs = [sendb[u, 0, 2 + sub, r, low : low + 16, :] for r in range(4)]
            for src in range(3):
                slabs += [recvb[u, src, sub, r, low : low + 16, :] for r in range(4)]
            out = jnp.dot(
                amat[part, g], jnp.concatenate(slabs, axis=0), preferred_element_type=F32
            )
            rows = slice((g % 4) * 128, (g % 4) * 128 + 128)
            if sub == 0:
                acc[u, rows, :] = out
            else:
                passb[u, rows, :] = out.astype(BF16)
        b_copy(u).start()

    def second_axis(u):
        part, axis, par = part_of(u)
        late = jnp.where(u >= LATE, 1, 0)
        return jnp.where(axis == 0, 1 - late, jnp.where(axis == 1, late, par))

    def to_second(u, v, sign):
        part, axis, par = part_of(u)
        a1, a2, a3 = coords(axis)
        swap = second_axis(u)
        old = jnp.where(swap == 0, a2, a3)
        new = (old + sign * v * (1 - 2 * (old % 2)) + 16) % 4
        return at(axis, a1, jnp.where(swap == 0, new, a2), jnp.where(swap == 0, a3, new), core)

    def to_third(u, v):
        part, axis, par = part_of(u)
        a1, a2, a3 = coords(axis)
        swap = second_axis(u)
        old = jnp.where(swap == 0, a3, a2)
        new = (old + v * (1 - 2 * (old % 2)) + 16) % 4
        return at(axis, a1, jnp.where(swap == 0, a2, new), jnp.where(swap == 0, new, a3), core)

    def turn(u):
        return (part_of(u)[2] + u // PARTS) % 2

    def c_copy(u):
        return remote(s2.at[u], r2.at[u], c_send, c_recv.at[u], to_second(u, 1, 1 - 2 * turn(u)))

    def phase_c(u):
        swap = second_axis(u)
        par = turn(u)
        all_in(passr.at[u], b_recv.at[u])

        def total(second, third):
            start = second * jnp.where(swap == 0, 128, 32) + third * jnp.where(swap == 0, 32, 128)
            rows = pl.ds(pl.multiple_of(start, 32), 32)
            return acc[u, rows, :] + passr[u, rows, :].astype(F32)

        for third in range(4):
            rows = slice(32 * third, 32 * third + 32)
            s2[u, 0, rows] = total(2 * par, third).astype(BF16)
            s2[u, 1, rows] = total(1, third).astype(BF16)
        c_copy(u).start()
        for third in range(4):
            rows = slice(32 * third, 32 * third + 32)
            acc2[u, 0, rows] = total(3, third)
            acc2[u, 1, rows] = total(2 - 2 * par, third)

    def h_copy(u):
        return remote(t2.at[u], q2.at[u], h_send, h_recv.at[u], to_second(u, 1, 2 * turn(u) - 1))

    def phase_h(u):
        all_in(r2.at[u], c_recv.at[u])
        t2[u] = (acc2[u, 1] + r2[u, 1].astype(F32)).astype(BF16)
        h_copy(u).start()
        acc2[u, 0] = acc2[u, 0] + r2[u, 0].astype(F32)

    def d_copies(u):
        return [
            remote(s3.at[u, d], r3.at[u, d], d_send, d_recv.at[u], to_third(u, d + 1))
            for d in range(3)
        ]

    def phase_d(u):
        all_in(q2.at[u], h_recv.at[u])
        total = acc2[u, 0] + q2[u].astype(F32)
        for d in range(3):
            s3[u, d] = total[32 * d : 32 * d + 32].astype(BF16)
        for copy in d_copies(u):
            copy.start()
        acc3[u] = total[96:128]

    me = blk * 2 + grp

    def e_copy(u, k):
        slot = (me - (u * 8 + k) + 255) % 128
        return remote(sp.at[u, k], rsp.at[slot], e_send, e_recv, (u * 4 + k // 2, k % 2))

    pair_rows = [(0, 0), (1, 0), (2, 0), (1, 6), (0, 2), (1, 2), (2, 2), (0, 4), (1, 4), (0, 6)]

    def e_sums(u):
        total = acc3[u]
        for d in range(3):
            total = total + r3[u, d].astype(F32)
        ell = (u * LANES + iota((32, 128), 1)).astype(F32)
        total = jnp.where(ell >= morder[...], total, 0.0)
        lanes = pl.ds(pl.multiple_of(u * LANES, LANES), LANES)
        harm_ref[:, lanes] = total
        heavy = total * mweight[...]
        near = [jnp.zeros((8, 128), F32) for _ in range(3)]
        for j in range(4):
            one = total[8 * j : 8 * j + 8]
            weighted = heavy[8 * j : 8 * j + 8]
            for k in range(3):
                other = one if k == 0 else pltpu.roll(one, 8 - 2 * k, 0)
                near[k] = near[k] + weighted * other
        near = [n + pltpu.roll(n, 7, 0) for n in near]
        lane = iota((8, 128), 1) >> 4
        packed = [jnp.zeros((8, 128), F32) for _ in range(2)]
        for p, (k, row) in enumerate(pair_rows):
            moved = near[k] if p % 8 == 0 else pltpu.roll(near[k], 16 * (p % 8), 1)
            wide = jnp.broadcast_to(moved[row : row + 1], (8, 128))
            wide = pltpu.roll(wide, 16, 1, stride=16, stride_axis=0)
            packed[p // 8] = jnp.where(lane == p % 8, wide, packed[p // 8])
        for k in range(8):
            for half in range(2):
                sp[u, k, half : half + 1, :] = packed[half][7 - k : 8 - k]

    def e_start(u):
        @pl.when(u != me // 8)
        def _():
            for k in range(8):
                e_copy(u, k).start()

        @pl.when(u == me // 8)
        def _():
            def send(k):
                @pl.when(k != me % 8)
                def _():
                    e_copy(u, k).start()

            loop(0, 8, send)

    def phase_e(lo, hi):
        for u in range(lo, hi):
            all_in(r3.at[u], d_recv.at[u])
        for u in range(lo, hi):
            e_sums(u)
            if u % 2:
                e_start(u - 1)
                e_start(u)

    def finish():
        arrived = remote(rsp, rsp, e_send, e_recv, device(x, y, z, 1 - core))
        arrived.wait_recv()
        sums = [sp[me // 8, me % 8], rsp[124], rsp[125], rsp[126]]
        for k in range(124):
            sums[k % 4] = sums[k % 4] + rsp[k]
        total = (sums[0] + sums[1]) + (sums[2] + sums[3])
        rows = []
        for half in range(2):
            wide = jnp.broadcast_to(total[half : half + 1], (8, 128))
            wide = pltpu.roll(wide, 16, 1, stride=16, stride_axis=0)
            rows += [wide[7 - p : 8 - p, 0:16] for p in range(8)]
        ell = me * 16 + iota((10, 16), 1)
        power = jnp.concatenate(rows[0:10], axis=0)
        spec_ref[...] = power / (2 * ell + 1).astype(F32)
        arrived.wait_send()

    def orders():
        mine = perm[0, 240:256, :].astype(F32)
        m = jnp.sum(mine * iota((16, 512), 1).astype(F32), axis=1, keepdims=True)
        m = jnp.broadcast_to(m, (16, 128))
        full = jnp.concatenate(
            [jnp.broadcast_to(m[j : j + 1], (8, 128)) for j in range(12, 16)], axis=0
        )
        morder[...] = full
        mweight[...] = jnp.where(full == 0.0, 1.0, 2.0)

    def phase(name, lo, hi, f):
        with jax.named_scope(name):
            loop(lo, hi, f)

    with jax.named_scope("a0"):
        perm_rows(0)
        a_rows(0)
        with jax.named_scope("meet"):
            pl.semaphore_wait(barrier, len(near_by))
        a_start(0)
        perm_rows(1)
        phase_a(2)
        phase_a(1)
        phase_a(3)
        perm_rows(2)
        loop(4, 6, phase_a)
    phase_a(6)
    phase_a(8)
    with jax.named_scope("fourier"):
        fourier()
        f_start()
    phase_a(7)
    phase("a2", 9, 16, phase_a)
    with jax.named_scope("orders"):
        orders()
    with jax.named_scope("build"):
        for part in (1, 3, 4, 5, 0, 2):
            build(part)
    phase("b0", 0, 6, phase_b)
    phase("b1", 6, 12, phase_b)
    phase("bX2", 12, 16, phase_b)
    phase("cX0", 0, 4, phase_c)
    phase("cZ0", 4, 6, phase_c)
    phase("cX1", 6, 10, phase_c)
    phase("cZ1", 10, 12, phase_c)
    phase("cX2", 12, 16, phase_c)
    phase("hX0", 0, 4, phase_h)
    phase("hZ0", 4, 6, phase_h)
    phase("hZ1", 10, 12, phase_h)
    phase("hX1", 6, 10, phase_h)
    phase("hX2", 12, 16, phase_h)
    phase("dX0", 0, 4, phase_d)
    phase("dZ0", 4, 6, phase_d)
    phase("dZ1", 10, 12, phase_d)
    phase("dX1", 6, 10, phase_d)
    phase("dX2", 12, 16, phase_d)
    for name, lo, hi in (("eX0", 0, 4), ("eZ0", 4, 6), ("eX1", 6, 10), ("eZ1", 10, 12), ("eX2", 12, 16)):
        with jax.named_scope(name):
            phase_e(lo, hi)
    with jax.named_scope("finish"):
        finish()

    with jax.named_scope("left"):
        all_out(frecv, f_send)
        all_out(recvb, a_send)
        all_out(passb, b_send)
        all_out(s2, c_send)
        all_out(t2, h_send)
        all_out(s3, d_send)


def per_device(sky_maps, legendre, owner_table, table, twiddle):
    vmem = pl.BlockSpec(memory_space=pltpu.VMEM)
    away = pl.BlockSpec(memory_space=pltpu.HBM)
    dma = pltpu.SemaphoreType.DMA
    V = pltpu.VMEM
    inputs = (sky_maps, legendre, owner_table.reshape(1, 512), table, twiddle)
    harm, spectra = pl.pallas_call(
        kernel,
        out_shape=(
            jax.ShapeDtypeStruct((32, 2048), F32),
            jax.ShapeDtypeStruct((10, 16), F32),
        ),
        in_specs=[away] * 5,
        out_specs=(vmem, vmem),
        scratch_shapes=[
            V((4, 4, 4096), F32),
            V((1, 512), jnp.int32),
            V((512, 1024), BF16),
            V((32, 2, 512), F32),
            V((UNITS, 4, 512, 128), BF16),
            V((UNITS, 2, 4, 4, 64, 128), BF16),
            V((UNITS, 3, 2, 4, 64, 128), BF16),
            V((3, 512, 512), BF16),
            V((PARTS, 8, 128, 256), BF16),
            V((512, 128), F32),
            V((512, 1024), F32),
            V((2, 16, 512), F32),
            V((32, 512), BF16),
            V((PARTS, 32, 128), BF16),
            V((PARTS, 3, 32, 128), BF16),
            V((PARTS, 3, 32, 128), BF16),
            V((UNITS, 512, 128), F32),
            V((UNITS, 512, 128), BF16),
            V((UNITS, 512, 128), BF16),
            V((UNITS, 2, 128, 128), F32),
            V((UNITS, 2, 128, 128), BF16),
            V((UNITS, 2, 128, 128), BF16),
            V((UNITS, 128, 128), BF16),
            V((UNITS, 128, 128), BF16),
            V((UNITS, 32, 128), F32),
            V((UNITS, 3, 32, 128), BF16),
            V((UNITS, 3, 32, 128), BF16),
            V((UNITS, 8, 2, 128), F32),
            V((127, 2, 128), F32),
            V((32, 128), F32),
            V((32, 128), F32),
            dma((4,)), dma((UNITS,)),
            dma, dma((UNITS,)), dma, dma((PARTS,)),
            dma, dma((UNITS,)), dma, dma((UNITS,)), dma, dma((UNITS,)), dma, dma((UNITS,)),
            dma, dma,
        ],
        compiler_params=pltpu.CompilerParams(
            collective_id=0, has_side_effects=True, vmem_limit_bytes=50 * 1024 * 1024
        ),
        name="analysis",
    )(*[pltpu.with_memory_space_constraint(v, pltpu.HBM) for v in inputs])
    return harm.reshape(4, 4, 2, 2048), spectra


def solution(mesh):
    both = ("blk", "grp")
    inner = jax.shard_map(
        per_device,
        mesh=mesh,
        in_specs=(P(None, both, None), P(both, None, None), P(), P(), P()),
        out_specs=(P(both, None, None, None), P(None, both)),
        check_vma=False,
    )

    def run(sky_maps, legendre, owner_table):
        table, twiddle = dft_tables()
        return inner(sky_maps, legendre, owner_table, jnp.asarray(table), jnp.asarray(twiddle))

    return run
```

```python
import functools
import math

import jax
import jax.numpy as jnp
import numpy as np
from jax import lax
from jax.experimental import pallas as pl
from jax.experimental.pallas import tpu as pltpu
from jax.sharding import PartitionSpec as P

MESH = pl.DeviceIdType.MESH
F32 = jnp.float32
BF16 = jnp.bfloat16
UNITS = 16
PARTS = 6
LANES = 128
LATE = 6


def iota(shape, dim):
    return lax.broadcasted_iota(jnp.int32, shape, dim)


def dft_tables():
    k2 = np.arange(128)[:, None]
    m = np.arange(512)[None, :]
    angle = 2.0 * math.pi * ((k2 * m) % 4096) / 4096.0
    table = np.concatenate([np.cos(angle), -np.sin(angle)], axis=1) / 64.0
    k1 = np.arange(32)[:, None]
    turn = 2.0 * math.pi * ((k1 * m) % 32) / 32.0
    twiddle = np.stack([np.cos(turn), np.sin(turn)], axis=1)
    table = table.astype(np.float32)
    high = table.astype(jnp.bfloat16)
    low = (table - high.astype(np.float32)).astype(jnp.bfloat16)
    lane = np.arange(1024)[None, :]
    spread = (lane >> 7) * 16 + (lane & 15) == np.arange(128)[:, None]
    diagonal = (np.arange(128)[:, None] >> 3) == (np.arange(128)[None, :] & 15)
    small = np.concatenate([spread, np.tile(diagonal, (1, 8))], axis=0).astype(jnp.bfloat16)
    return np.concatenate([high, low, small], axis=0), twiddle.astype(np.float32)


def kernel(
    sky_in, leg_ref, own_in, table_in, twid_in, harm_ref, spec_ref,
    sky_ref, own_ref, table_ref, twid_ref, legv, sendb, recvb, perm, amat, fx, fz, fre, fown, fkeep, fsend, frecv,
    acc, passb, passr, acc2, s2, r2, t2, q2, acc3, s3, r3, sp, rsp, morder, mweight,
    in_sem, leg_sem, a_send, a_recv, f_send, f_recv, b_send, b_recv, c_send, c_recv,
    h_send, h_recv, d_send, d_recv, e_send, e_recv,
):
    blk = lax.axis_index("blk")
    grp = lax.axis_index("grp")
    x = blk // 16
    y = (blk // 4) % 4
    z = grp * 2 + (blk // 2) % 2
    core = blk % 2

    def pick(axis, v0, v1, v2):
        return jnp.where(axis == 0, v0, jnp.where(axis == 1, v1, v2))

    def coords(axis):
        return pick(axis, x, y, z), pick(axis, y, z, x), pick(axis, z, x, y)

    def device(xx, yy, zz, cc):
        return (xx * 16 + yy * 4 + (zz % 2) * 2 + cc, zz // 2)

    def at(axis, v1, v2, v3, cc):
        return device(pick(axis, v1, v3, v2), pick(axis, v2, v1, v3), pick(axis, v3, v2, v1), cc)

    def part_of(u, c=core):
        late = jnp.where(u == 12, 0, jnp.where(u == 13, 1 + 2 * c, jnp.where(u == 14, 2, 4 + c)))
        part = jnp.where(u < 12, u % PARTS, late)
        return part, part // 2, part % 2

    def pairs(axis, par):
        a1, a2, a3 = coords(axis)
        step = (1 - 2 * (a1 % 2)) * (1 - 2 * par)
        first = (a1 + step + 4) % 4
        second = (a1 - step + 4) % 4
        return a1, a2, a3, first, second

    def remote(src, dst, ss, rs, dev):
        return pltpu.make_async_remote_copy(
            src_ref=src, dst_ref=dst, send_sem=ss, recv_sem=rs, device_id=dev, device_id_type=MESH
        )

    def loop(lo, hi, f):
        def body(i, c):
            f(i)
            return c

        lax.fori_loop(lo, hi, body, 0)

    barrier = pltpu.get_barrier_semaphore()
    near_by = [device(x, y, z, 1 - core)]
    for axis in range(3):
        a1, a2, a3 = coords(axis)
        for d in (1, 2, 3):
            near_by.append(at(axis, (a1 + d) % 4, a2, a3, core))
            if d != 2:
                near_by.append(at(axis, (a1 + d) % 4, a2, a3, 1 - core))
    for dev in near_by:
        pl.semaphore_signal(barrier, inc=1, device_id=dev, device_id_type=MESH)

    def leg_copy(u):
        lanes = pl.ds(pl.multiple_of(u * LANES, LANES), LANES)
        return pltpu.make_async_copy(leg_ref.at[:, :, lanes], legv.at[u], leg_sem.at[u])

    inputs = [
        pltpu.make_async_copy(src, dst, in_sem.at[i])
        for i, (src, dst) in enumerate(
            [(own_in, own_ref), (sky_in, sky_ref), (table_in, table_ref), (twid_in, twid_ref)]
        )
    ]
    inputs[0].start()
    loop(0, PARTS, lambda u: leg_copy(u).start())
    for copy in inputs[1:]:
        copy.start()
    loop(PARTS, UNITS, lambda u: leg_copy(u).start())

    def perm_rows(axis):
        a1, a2, a3 = coords(axis)
        i = iota((512, 128), 0)
        v3 = (a3 + ((i >> 2) + 1) * (1 - 2 * (a3 % 2)) + 512) & 3
        v2 = (a2 + ((i >> 4) + 1) * (1 - 2 * (a2 % 2)) + 128) & 3
        v1 = (a1 + (((i >> 6) & 3) + 1) * (1 - 2 * (a1 % 2)) + 16) & 3
        cc = core ^ (i >> 8)
        xx, yy, zz = ((v1, v2, v3), (v3, v1, v2), (v2, v3, v1))[axis]
        slot = (xx << 7) + (yy << 5) + ((zz & 1) << 4) + (cc << 3) + ((zz >> 1) << 2) + (i & 3)
        slot = slot - iota((512, 128), 1)
        chosen = jnp.concatenate(
            [jnp.where(slot == k * 128, 1.0, 0.0).astype(BF16) for k in range(4)], axis=1
        )
        if axis == 0:
            inputs[0].wait()
        order = own_ref[...]
        row = iota((8, 512), 0)
        digits = jnp.where(row == 0, order & 255, jnp.where(row == 1, order >> 8, 0))
        codes = lax.dot_general(
            chosen, digits.astype(F32).astype(BF16), (((1,), (1,)), ((), ())),
            preferred_element_type=F32,
        )
        orders_of = codes[:, 0:1] + 256.0 * codes[:, 1:2]
        for k in range(4):
            m = (iota((512, 128), 1) + k * 128).astype(F32)
            perm[axis, :, k * 128 : k * 128 + 128] = jnp.where(m == orders_of, 1.0, 0.0).astype(BF16)

    def a_copies(u):
        part, axis, par = part_of(u)
        a1, a2, a3, first, _ = pairs(axis, par)
        _, axis_o, par_o = part_of(u, 1 - core)
        _, b2, b3, first_o, _ = pairs(axis_o, par_o)
        sem = a_recv.at[u]
        return (
            remote(sendb.at[u, 0, pl.ds(0, 2)], recvb.at[u, 1], a_send, sem,
                   at(axis, first, a2, a3, core)),
            remote(sendb.at[u, 1, pl.ds(0, 2)], recvb.at[u, 2], a_send, sem,
                   at(axis_o, first_o, b2, b3, 1 - core)),
            remote(sendb.at[u, 1, pl.ds(2, 2)], recvb.at[u, 0], a_send, sem,
                   device(x, y, z, 1 - core)),
        )

    def a_rows(u):
        leg_copy(u).wait()
        kinds = [part_of(u, core), part_of(u, 1 - core)]
        for pair in range(2):
            wide = jnp.concatenate([legv[u, 2 * pair], legv[u, 2 * pair + 1]], axis=1)
            for rc, (_, axis, par) in enumerate(kinds):
                roles = (3 * par, 1, 3 - 3 * par, 2)
                chosen = perm[axis, rc * 256 : rc * 256 + 256, :]
                rows = jnp.dot(chosen, wide, preferred_element_type=F32).astype(BF16)
                for rel in range(4):
                    piece = rows[rel * 64 : rel * 64 + 64]
                    sendb[u, rc, roles[rel], 2 * pair] = piece[:, :128]
                    sendb[u, rc, roles[rel], 2 * pair + 1] = piece[:, 128:]

    def a_start(u):
        for copy in a_copies(u):
            copy.start()

    def phase_a(u):
        a_rows(u)
        a_start(u)

    def all_in(ref, sem):
        remote(ref, ref, a_send, sem, device(x, y, z, 1 - core)).wait_recv()

    def all_out(ref, sem):
        remote(ref, ref, sem, e_recv, device(x, y, z, 1 - core)).wait_send()

    def fourier():
        for copy in inputs[1:]:
            copy.wait()
        for a in range(4):
            for k1 in range(32):
                fx[k1 * 16 + a * 4 : k1 * 16 + a * 4 + 4, :] = sky_ref[
                    a, :, k1 * 128 : (k1 + 1) * 128
                ]

        def rows_of(i):
            rows = pl.ds(pl.multiple_of(i * 128, 128), 128)
            pixels = fx[rows, :]
            high = pixels.astype(BF16)
            low = (pixels - high.astype(F32)).astype(BF16)
            table = table_ref[0:128, :]
            fz[rows, :] = jnp.dot(
                jnp.concatenate([high, low], axis=1), jnp.concatenate([table, table], axis=0),
                preferred_element_type=F32,
            ) + jnp.dot(high, table_ref[128:256, :], preferred_element_type=F32)

        for i in range(4):
            rows_of(i)

        def add(k1, sums):
            re, im = sums
            rows = pl.ds(pl.multiple_of(k1 * 16, 16), 16)
            zr = fz[rows, 0:512]
            zi = fz[rows, 512:1024]
            c = twid_ref[k1, 0:1, :]
            s = twid_ref[k1, 1:2, :]
            return re + (zr * c + zi * s), im + (zi * c - zr * s)

        zero = jnp.zeros((16, 512), F32)
        re, im = lax.fori_loop(0, 32, add, (zero, zero), unroll=8)
        fre[0] = re
        fre[1] = im
        for r in range(4):
            rows = [fre[q, a * 4 + r : a * 4 + r + 1, :] for a in range(4) for q in range(2)]
            fown[r * 8 : r * 8 + 8, :] = jnp.concatenate(rows, axis=0).astype(BF16)

    def f_copies(part):
        axis, par = part // 2, part % 2
        a1, a2, a3, first, _ = pairs(axis, par)
        sem = f_recv.at[part]
        return (
            remote(fsend.at[part, 0], frecv.at[part, 1], f_send, sem, at(axis, first, a2, a3, core)),
            remote(fsend.at[part, 1], frecv.at[part, 2], f_send, sem,
                   at(axis, first, a2, a3, 1 - core)),
            remote(fsend.at[part, 2], frecv.at[part, 0], f_send, sem,
                   at(axis, a1, a2, a3, 1 - core)),
        )

    def f_start():
        low = iota((32, 128), 1) < 64
        for axis in range(3):
            cols = lax.dot_general(
                fown[...], perm[axis], (((1,), (1,)), ((), ())), preferred_element_type=F32
            )
            tile = [cols[:, k * 128 : k * 128 + 128] for k in range(4)]
            turned = [pltpu.roll(t, 64, 1) for t in tile]

            def half(rel, rc, side):
                return (tile if rel % 2 == side else turned)[2 * rc + rel // 2]

            def joined(mine, passed, rc):
                return jnp.where(low, half(mine, rc, 0), half(passed, rc, 1)).astype(BF16)

            for par in range(2):
                part = 2 * axis + par
                fsend[part, 0] = joined(2 * par, 1, 0)
                fsend[part, 1] = joined(2 * par, 1, 1)
                fsend[part, 2] = joined(3, 2 - 2 * par, 1)
                fkeep[part] = joined(3, 2 - 2 * par, 0)
                for copy in f_copies(part):
                    copy.start()

    def build(part):
        all_in(frecv.at[part], f_recv.at[part])
        picked = jnp.concatenate([fkeep[part]] + [frecv[part, k] for k in range(3)], axis=0)
        tiled = jnp.dot(picked, table_ref[256:384, :], preferred_element_type=F32)
        group = iota((8, 128), 1) >> 4
        for g in range(8):
            for h in range(2):
                base = tiled[64 * h : 64 * h + 8, g * 128 : g * 128 + 128]
                for i in range(1, 8):
                    row = (8 * h + i) * 8
                    base = jnp.where(
                        group == i, tiled[row : row + 8, g * 128 : g * 128 + 128], base
                    )
                two = jnp.concatenate([base, base], axis=0).astype(BF16)
                for k in range(8):
                    rows = slice(16 * k, 16 * k + 16)
                    amat[part, g, rows, h * 128 : h * 128 + 128] = (
                        two * table_ref[384 + 16 * k : 400 + 16 * k, 0:128]
                    )

    def b_copy(u):
        part, axis, par = part_of(u)
        _, a2, a3, _, second = pairs(axis, par)
        return remote(passb.at[u], passr.at[u], b_send, b_recv.at[u],
                      at(axis, second, a2, a3, core))

    def phase_b(u):
        part, axis, par = part_of(u)
        all_in(recvb.at[u], a_recv.at[u])
        for g in (4, 5, 6, 7, 0, 1, 2, 3):
            sub, low = g // 4, 16 * (g % 4)
            slabs = [sendb[u, 0, 2 + sub, r, low : low + 16, :] for r in range(4)]
            for src in range(3):
                slabs += [recvb[u, src, sub, r, low : low + 16, :] for r in range(4)]
            out = jnp.dot(
                amat[part, g], jnp.concatenate(slabs, axis=0), preferred_element_type=F32
            )
            rows = slice((g % 4) * 128, (g % 4) * 128 + 128)
            if sub == 0:
                acc[u, rows, :] = out
            else:
                passb[u, rows, :] = out.astype(BF16)
            if g == 7:
                b_copy(u).start()

    def second_axis(u):
        part, axis, par = part_of(u)
        late = jnp.where(u >= LATE, 1, 0)
        return jnp.where(axis == 0, 1 - late, jnp.where(axis == 1, late, par))

    def to_second(u, v, sign):
        part, axis, par = part_of(u)
        a1, a2, a3 = coords(axis)
        swap = second_axis(u)
        old = jnp.where(swap == 0, a2, a3)
        new = (old + sign * v * (1 - 2 * (old % 2)) + 16) % 4
        return at(axis, a1, jnp.where(swap == 0, new, a2), jnp.where(swap == 0, a3, new), core)

    def to_third(u, v):
        part, axis, par = part_of(u)
        a1, a2, a3 = coords(axis)
        swap = second_axis(u)
        old = jnp.where(swap == 0, a3, a2)
        new = (old + v * (1 - 2 * (old % 2)) + 16) % 4
        return at(axis, a1, jnp.where(swap == 0, a2, new), jnp.where(swap == 0, new, a3), core)

    def turn(u):
        return (part_of(u)[2] + u // PARTS) % 2

    def c_copy(u):
        return remote(s2.at[u], r2.at[u], c_send, c_recv.at[u], to_second(u, 1, 1 - 2 * turn(u)))

    def phase_c(u):
        swap = second_axis(u)
        par = turn(u)
        all_in(passr.at[u], b_recv.at[u])

        def total(second, third):
            start = second * jnp.where(swap == 0, 128, 32) + third * jnp.where(swap == 0, 32, 128)
            rows = pl.ds(pl.multiple_of(start, 32), 32)
            return acc[u, rows, :] + passr[u, rows, :].astype(F32)

        for third in range(4):
            rows = slice(32 * third, 32 * third + 32)
            s2[u, 0, rows] = total(2 * par, third).astype(BF16)
            s2[u, 1, rows] = total(1, third).astype(BF16)
        c_copy(u).start()
        for third in range(4):
            rows = slice(32 * third, 32 * third + 32)
            acc2[u, 0, rows] = total(3, third)
            acc2[u, 1, rows] = total(2 - 2 * par, third)

    def h_copy(u):
        return remote(t2.at[u], q2.at[u], h_send, h_recv.at[u], to_second(u, 1, 2 * turn(u) - 1))

    def phase_h(u):
        all_in(r2.at[u], c_recv.at[u])
        t2[u] = (acc2[u, 1] + r2[u, 1].astype(F32)).astype(BF16)
        h_copy(u).start()
        acc2[u, 0] = acc2[u, 0] + r2[u, 0].astype(F32)

    def d_copies(u):
        return [
            remote(s3.at[u, d], r3.at[u, d], d_send, d_recv.at[u], to_third(u, d + 1))
            for d in range(3)
        ]

    def phase_d(u):
        all_in(q2.at[u], h_recv.at[u])
        total = acc2[u, 0] + q2[u].astype(F32)
        for d in range(3):
            s3[u, d] = total[32 * d : 32 * d + 32].astype(BF16)
        for copy in d_copies(u):
            copy.start()
        acc3[u] = total[96:128]

    me = blk * 2 + grp

    def e_copy(u, k):
        slot = (me - (u * 8 + k) + 255) % 128
        return remote(sp.at[u, k], rsp.at[slot], e_send, e_recv, (u * 4 + k // 2, k % 2))

    pair_rows = [(0, 0), (1, 0), (2, 0), (1, 6), (0, 2), (1, 2), (2, 2), (0, 4), (1, 4), (0, 6)]

    def e_sums(u):
        total = acc3[u]
        for d in range(3):
            total = total + r3[u, d].astype(F32)
        ell = (u * LANES + iota((32, 128), 1)).astype(F32)
        total = jnp.where(ell >= morder[...], total, 0.0)
        lanes = pl.ds(pl.multiple_of(u * LANES, LANES), LANES)
        harm_ref[:, lanes] = total
        heavy = total * mweight[...]
        near = [jnp.zeros((8, 128), F32) for _ in range(3)]
        for j in range(4):
            one = total[8 * j : 8 * j + 8]
            weighted = heavy[8 * j : 8 * j + 8]
            for k in range(3):
                other = one if k == 0 else pltpu.roll(one, 8 - 2 * k, 0)
                near[k] = near[k] + weighted * other
        near = [n + pltpu.roll(n, 7, 0) for n in near]
        lane = iota((8, 128), 1) >> 4
        packed = [jnp.zeros((8, 128), F32) for _ in range(2)]
        for p, (k, row) in enumerate(pair_rows):
            moved = near[k] if p % 8 == 0 else pltpu.roll(near[k], 16 * (p % 8), 1)
            wide = jnp.broadcast_to(moved[row : row + 1], (8, 128))
            wide = pltpu.roll(wide, 16, 1, stride=16, stride_axis=0)
            packed[p // 8] = jnp.where(lane == p % 8, wide, packed[p // 8])
        for k in range(8):
            for half in range(2):
                sp[u, k, half : half + 1, :] = packed[half][7 - k : 8 - k]

    def e_start(u):
        @pl.when(u != me // 8)
        def _():
            for k in range(8):
                e_copy(u, k).start()

        @pl.when(u == me // 8)
        def _():
            def send(k):
                @pl.when(k != me % 8)
                def _():
                    e_copy(u, k).start()

            loop(0, 8, send)

    def phase_e(lo, hi):
        for u in range(lo, hi):
            all_in(r3.at[u], d_recv.at[u])
        for u in range(lo, hi):
            e_sums(u)
            if u % 2:
                e_start(u - 1)
                e_start(u)

    def finish():
        arrived = remote(rsp, rsp, e_send, e_recv, device(x, y, z, 1 - core))
        arrived.wait_recv()
        sums = [sp[me // 8, me % 8], rsp[124], rsp[125], rsp[126]]
        for k in range(124):
            sums[k % 4] = sums[k % 4] + rsp[k]
        total = (sums[0] + sums[1]) + (sums[2] + sums[3])
        rows = []
        for half in range(2):
            wide = jnp.broadcast_to(total[half : half + 1], (8, 128))
            wide = pltpu.roll(wide, 16, 1, stride=16, stride_axis=0)
            rows += [wide[7 - p : 8 - p, 0:16] for p in range(8)]
        ell = me * 16 + iota((10, 16), 1)
        power = jnp.concatenate(rows[0:10], axis=0)
        spec_ref[...] = power / (2 * ell + 1).astype(F32)
        arrived.wait_send()

    def orders():
        mine = perm[0, 240:256, :].astype(F32)
        m = jnp.sum(mine * iota((16, 512), 1).astype(F32), axis=1, keepdims=True)
        m = jnp.broadcast_to(m, (16, 128))
        full = jnp.concatenate(
            [jnp.broadcast_to(m[j : j + 1], (8, 128)) for j in range(12, 16)], axis=0
        )
        morder[...] = full
        mweight[...] = jnp.where(full == 0.0, 1.0, 2.0)

    def phase(name, lo, hi, f):
        with jax.named_scope(name):
            loop(lo, hi, f)

    with jax.named_scope("a0"):
        perm_rows(0)
        a_rows(0)
        with jax.named_scope("meet"):
            pl.semaphore_wait(barrier, len(near_by))
        a_start(0)
        perm_rows(1)
        phase_a(2)
        phase_a(1)
        phase_a(3)
        perm_rows(2)
        loop(4, 6, phase_a)
    phase_a(6)
    phase_a(8)
    with jax.named_scope("fourier"):
        fourier()
        f_start()
    phase_a(7)
    phase("a2", 9, 16, phase_a)
    with jax.named_scope("orders"):
        orders()
    with jax.named_scope("build"):
        for part in (1, 3, 4, 5, 0, 2):
            build(part)
    phase("b0", 0, 6, phase_b)
    phase("b1", 6, 12, phase_b)
    phase("bX2", 12, 16, phase_b)
    phase("cX0", 0, 4, phase_c)
    phase("cZ0", 4, 6, phase_c)
    phase("cX1", 6, 10, phase_c)
    phase("cZ1", 10, 12, phase_c)
    phase("cX2", 12, 16, phase_c)
    phase("hX0", 0, 4, phase_h)
    phase("hZ0", 4, 6, phase_h)
    phase("hZ1", 10, 12, phase_h)
    phase("hX1", 6, 10, phase_h)
    phase("hX2", 12, 16, phase_h)
    phase("dX0", 0, 4, phase_d)
    phase("dZ0", 4, 6, phase_d)
    phase("dZ1", 10, 12, phase_d)
    phase("dX1", 6, 10, phase_d)
    phase("dX2", 12, 16, phase_d)
    for name, lo, hi in (("eX0", 0, 4), ("eZ0", 4, 6), ("eX1", 6, 10), ("eZ1", 10, 12), ("eX2", 12, 16)):
        with jax.named_scope(name):
            phase_e(lo, hi)
    with jax.named_scope("finish"):
        finish()

    with jax.named_scope("left"):
        all_out(frecv, f_send)
        all_out(recvb, a_send)
        all_out(passb, b_send)
        all_out(s2, c_send)
        all_out(t2, h_send)
        all_out(s3, d_send)


def per_device(sky_maps, legendre, owner_table, table, twiddle):
    vmem = pl.BlockSpec(memory_space=pltpu.VMEM)
    away = pl.BlockSpec(memory_space=pltpu.HBM)
    dma = pltpu.SemaphoreType.DMA
    V = pltpu.VMEM
    inputs = (sky_maps, legendre, owner_table.reshape(1, 512), table, twiddle)
    harm, spectra = pl.pallas_call(
        kernel,
        out_shape=(
            jax.ShapeDtypeStruct((32, 2048), F32),
            jax.ShapeDtypeStruct((10, 16), F32),
        ),
        in_specs=[away] * 5,
        out_specs=(vmem, vmem),
        scratch_shapes=[
            V((4, 4, 4096), F32),
            V((1, 512), jnp.int32),
            V((512, 1024), BF16),
            V((32, 2, 512), F32),
            V((UNITS, 4, 512, 128), BF16),
            V((UNITS, 2, 4, 4, 64, 128), BF16),
            V((UNITS, 3, 2, 4, 64, 128), BF16),
            V((3, 512, 512), BF16),
            V((PARTS, 8, 128, 256), BF16),
            V((512, 128), F32),
            V((512, 1024), F32),
            V((2, 16, 512), F32),
            V((32, 512), BF16),
            V((PARTS, 32, 128), BF16),
            V((PARTS, 3, 32, 128), BF16),
            V((PARTS, 3, 32, 128), BF16),
            V((UNITS, 512, 128), F32),
            V((UNITS, 512, 128), BF16),
            V((UNITS, 512, 128), BF16),
            V((UNITS, 2, 128, 128), F32),
            V((UNITS, 2, 128, 128), BF16),
            V((UNITS, 2, 128, 128), BF16),
            V((UNITS, 128, 128), BF16),
            V((UNITS, 128, 128), BF16),
            V((UNITS, 32, 128), F32),
            V((UNITS, 3, 32, 128), BF16),
            V((UNITS, 3, 32, 128), BF16),
            V((UNITS, 8, 2, 128), F32),
            V((127, 2, 128), F32),
            V((32, 128), F32),
            V((32, 128), F32),
            dma((4,)), dma((UNITS,)),
            dma, dma((UNITS,)), dma, dma((PARTS,)),
            dma, dma((UNITS,)), dma, dma((UNITS,)), dma, dma((UNITS,)), dma, dma((UNITS,)),
            dma, dma,
        ],
        compiler_params=pltpu.CompilerParams(
            collective_id=0, has_side_effects=True, vmem_limit_bytes=50 * 1024 * 1024
        ),
        name="analysis",
    )(*[pltpu.with_memory_space_constraint(v, pltpu.HBM) for v in inputs])
    return harm.reshape(4, 4, 2, 2048), spectra


def solution(mesh):
    both = ("blk", "grp")
    inner = jax.shard_map(
        per_device,
        mesh=mesh,
        in_specs=(P(None, both, None), P(both, None, None), P(), P(), P()),
        out_specs=(P(both, None, None, None), P(None, both)),
        check_vma=False,
    )

    def run(sky_maps, legendre, owner_table):
        table, twiddle = dft_tables()
        return inner(sky_maps, legendre, owner_table, jnp.asarray(table), jnp.asarray(twiddle))

    return run
```
